8 devices in a mesh: part: 1 (over z), dp: 8 (over y, x, core).
Axes of the slice: x: 2, y: 2, z: 1, core: 2. Of those that a mesh axis runs over, the one named last changes fastest.
Arguments:
- hidden: bfloat16 [32, 512, 2048], P(('part', 'dp'))
- prompt_lens: int32 [32], P(('part', 'dp'))
- g_attn: bfloat16 [2, 2048], P(None, 'dp')
- w_query: bfloat16 [2, 2048, 32, 64], P(None, 'dp')
- w_key: bfloat16 [2, 2048, 32, 64], P(None, 'dp')
- w_value: bfloat16 [2, 2048, 32, 64], P(None, 'dp')
- w_out: bfloat16 [2, 2048, 2048], P(None, 'dp')
- g_mlp: bfloat16 [2, 2048], P(None, 'dp')
- w_gate: bfloat16 [2, 2048, 8192], P(None, 'dp')
- w_up: bfloat16 [2, 2048, 8192], P(None, 'dp')
- w_down: bfloat16 [2, 8192, 2048], P(None, 'dp')
- g_final: bfloat16 [2048], P('dp')
- embedding: bfloat16 [49152, 2048], P('dp')
Outputs:
- output 1: bfloat16 [2, 32, 512, 32, 64], P(None, ('part', 'dp'))
- output 2: bfloat16 [2, 32, 512, 32, 64], P(None, ('part', 'dp'))
- output 3: float32 [32, 49152], P(('part', 'dp'))
All inputs are finite; a program needn't handle non-finite values.
Results may differ from the reference program's by a relative error of at most 0.0160224.
Values are sent between devices in bfloat16 or wider.
A program may use at most 1 GiB of HBM per device.

```python
import math
import jax
import jax.numpy as jnp
from jax import lax

BATCH_ROWS = 32
SEQ_LEN = 512
MODEL_DIM = 2048
NUM_HEADS = 32
KV_HEADS = 32
HEAD_DIM = 64
FFN_DIM = 8192
VOCAB_SIZE = 49152
LAYERS = 2
GROUP_SIZE = NUM_HEADS // KV_HEADS


def draw_normal(rng_key, arr_shape, fan_in):
    return (jax.random.normal(rng_key, arr_shape, jnp.float32) * fan_in ** -0.5).astype(jnp.bfloat16)


def draw_gain(rng_key, arr_shape):
    return jax.random.uniform(rng_key, arr_shape, jnp.float32, 0.5, 1.5).astype(jnp.bfloat16)


def setup_inputs(seed: int = 0, part: int = 0) -> dict:
    part_key = jax.random.fold_in(jax.random.key(seed), part)
    act_key, len_key = jax.random.split(part_key)
    weight_keys = jax.random.split(jax.random.key(seed + 1), 11)
    hidden = jax.random.normal(act_key, (BATCH_ROWS, SEQ_LEN, MODEL_DIM), jnp.float32).astype(jnp.bfloat16)
    drawn_lens = jax.random.randint(len_key, (BATCH_ROWS,), 1, SEQ_LEN + 1, jnp.int32)
    prompt_lens = drawn_lens.at[0].set(SEQ_LEN).at[BATCH_ROWS - 1].set(1)
    return {
        "hidden": hidden,
        "prompt_lens": prompt_lens,
        "g_attn": draw_gain(weight_keys[0], (LAYERS, MODEL_DIM)),
        "w_query": draw_normal(weight_keys[1], (LAYERS, MODEL_DIM, NUM_HEADS, HEAD_DIM), MODEL_DIM),
        "w_key": draw_normal(weight_keys[2], (LAYERS, MODEL_DIM, KV_HEADS, HEAD_DIM), MODEL_DIM),
        "w_value": draw_normal(weight_keys[3], (LAYERS, MODEL_DIM, KV_HEADS, HEAD_DIM), MODEL_DIM),
        "w_out": draw_normal(weight_keys[4], (LAYERS, NUM_HEADS * HEAD_DIM, MODEL_DIM), NUM_HEADS * HEAD_DIM),
        "g_mlp": draw_gain(weight_keys[5], (LAYERS, MODEL_DIM)),
        "w_gate": draw_normal(weight_keys[6], (LAYERS, MODEL_DIM, FFN_DIM), MODEL_DIM),
        "w_up": draw_normal(weight_keys[7], (LAYERS, MODEL_DIM, FFN_DIM), MODEL_DIM),
        "w_down": draw_normal(weight_keys[8], (LAYERS, FFN_DIM, MODEL_DIM), FFN_DIM),
        "g_final": draw_gain(weight_keys[9], (MODEL_DIM,)),
        "embedding": draw_normal(weight_keys[10], (VOCAB_SIZE, MODEL_DIM), MODEL_DIM),
    }


def rope_tables(seq_len, head_dim):
    half_dim = head_dim // 2
    exponent = jnp.arange(half_dim, dtype=jnp.float32) * (2.0 / head_dim)
    inv_freq = 1.0 / (500000.0 ** exponent)
    wave_len = 2.0 * math.pi / inv_freq
    smooth = (8192.0 / wave_len - 1.0) / 3.0
    blended = (1.0 - smooth) * inv_freq / 8.0 + smooth * inv_freq
    scaled = jnp.where(wave_len > 8192.0, inv_freq / 8.0, jnp.where(wave_len < 2048.0, inv_freq, blended))
    angles = jnp.arange(seq_len, dtype=jnp.float32)[:, None] * scaled[None, :]
    return jnp.cos(angles), jnp.sin(angles)


def apply_rope(values, cos_tab, sin_tab):
    half_dim = values.shape[-1] // 2
    low_half = values[..., :half_dim]
    high_half = values[..., half_dim:]
    cos_view = cos_tab[:, None, :]
    sin_view = sin_tab[:, None, :]
    return jnp.concatenate([low_half * cos_view - high_half * sin_view, high_half * cos_view + low_half * sin_view], axis=-1)


def rms_norm(values, gain_vec):
    values_f32 = values.astype(jnp.float32)
    mean_sq = jnp.mean(values_f32 * values_f32, axis=-1, keepdims=True)
    return (values_f32 * lax.rsqrt(mean_sq + 1e-5) * gain_vec.astype(jnp.float32)).astype(jnp.bfloat16)


def layer_row(hidden_row, length, layer_params, cos_tab, sin_tab):
    g_attn, w_query, w_key, w_value, w_out, g_mlp, w_gate, w_up, w_down = layer_params
    normed = rms_norm(hidden_row, g_attn)
    query_lin = jnp.dot(normed, w_query.reshape(MODEL_DIM, NUM_HEADS * HEAD_DIM), preferred_element_type=jnp.float32)
    query_rot = apply_rope(query_lin.reshape(SEQ_LEN, NUM_HEADS, HEAD_DIM), cos_tab, sin_tab).astype(jnp.bfloat16)
    query_rot = query_rot.reshape(SEQ_LEN, KV_HEADS, GROUP_SIZE, HEAD_DIM)
    key_lin = jnp.dot(normed, w_key.reshape(MODEL_DIM, KV_HEADS * HEAD_DIM), preferred_element_type=jnp.float32)
    key_rot = apply_rope(key_lin.reshape(SEQ_LEN, KV_HEADS, HEAD_DIM), cos_tab, sin_tab).astype(jnp.bfloat16)
    value_vec = jnp.dot(normed, w_value.reshape(MODEL_DIM, KV_HEADS * HEAD_DIM), preferred_element_type=jnp.float32)
    value_vec = value_vec.astype(jnp.bfloat16).reshape(SEQ_LEN, KV_HEADS, HEAD_DIM)
    scores = jnp.einsum("skgd,tkd->kgst", query_rot.astype(jnp.float32), key_rot.astype(jnp.float32)) * HEAD_DIM ** -0.5
    positions = jnp.arange(SEQ_LEN)
    allowed = (positions[None, :] <= positions[:, None]) & (positions[None, :] < length)
    scores = jnp.where(allowed, scores, -jnp.inf)
    row_max = jnp.max(scores, axis=-1, keepdims=True)
    exp_scores = jnp.exp(scores - row_max)
    attn_probs = (exp_scores / jnp.sum(exp_scores, axis=-1, keepdims=True)).astype(jnp.bfloat16)
    attended = jnp.einsum("kgst,tkd->skgd", attn_probs.astype(jnp.float32), value_vec.astype(jnp.float32))
    attended = attended.astype(jnp.bfloat16).reshape(SEQ_LEN, NUM_HEADS * HEAD_DIM)
    hidden_mid = (hidden_row.astype(jnp.float32) + jnp.dot(attended, w_out, preferred_element_type=jnp.float32)).astype(jnp.bfloat16)
    normed_mlp = rms_norm(hidden_mid, g_mlp)
    gate_val = jnp.dot(normed_mlp, w_gate, preferred_element_type=jnp.float32)
    up_val = jnp.dot(normed_mlp, w_up, preferred_element_type=jnp.float32)
    mlp_act = (jax.nn.silu(gate_val) * up_val).astype(jnp.bfloat16)
    hidden_out = (hidden_mid.astype(jnp.float32) + jnp.dot(mlp_act, w_down, preferred_element_type=jnp.float32)).astype(jnp.bfloat16)
    return hidden_out, (key_rot, value_vec)


def reference(hidden, prompt_lens, g_attn, w_query, w_key, w_value, w_out, g_mlp, w_gate, w_up, w_down, g_final, embedding):
    cos_tab, sin_tab = rope_tables(SEQ_LEN, HEAD_DIM)
    stacked = (g_attn, w_query, w_key, w_value, w_out, g_mlp, w_gate, w_up, w_down)

    def one_prompt(prompt):
        hidden_row, length = prompt

        def layer_step(carry_row, layer_params):
            return layer_row(carry_row, length, layer_params, cos_tab, sin_tab)

        final_row, cache_pair = lax.scan(layer_step, hidden_row, stacked)
        last_row = lax.dynamic_index_in_dim(final_row, length - 1, axis=0, keepdims=False)
        return last_row, cache_pair[0], cache_pair[1]

    last_rows, key_rows, value_rows = lax.map(one_prompt, (hidden, prompt_lens))
    normed_last = rms_norm(last_rows, g_final)
    logits = jnp.dot(normed_last, embedding.T, preferred_element_type=jnp.float32)
    return jnp.swapaxes(key_rows, 0, 1), jnp.swapaxes(value_rows, 0, 1), logits
```

```python
import math
import jax
import jax.numpy as jnp
from jax import lax
from jax.sharding import PartitionSpec as P

F32 = jnp.float32
BF16 = jnp.bfloat16


def rope_tables(seq_len, head_dim):
    half_dim = head_dim // 2
    exponent = jnp.arange(half_dim, dtype=jnp.float32) * (2.0 / head_dim)
    inv_freq = 1.0 / (500000.0 ** exponent)
    wave_len = 2.0 * math.pi / inv_freq
    smooth = (8192.0 / wave_len - 1.0) / 3.0
    blended = (1.0 - smooth) * inv_freq / 8.0 + smooth * inv_freq
    scaled = jnp.where(wave_len > 8192.0, inv_freq / 8.0, jnp.where(wave_len < 2048.0, inv_freq, blended))
    angles = jnp.arange(seq_len, dtype=jnp.float32)[:, None] * scaled[None, :]
    return jnp.cos(angles), jnp.sin(angles)


def rms_norm(values, gain_f32):
    values_f32 = values.astype(F32)
    mean_sq = jnp.mean(values_f32 * values_f32, axis=-1, keepdims=True)
    return (values_f32 * lax.rsqrt(mean_sq + 1e-5) * gain_f32).astype(BF16)


def rope_bhes(x, cos_es, sin_es):
    half = x.shape[2] // 2
    low, high = x[:, :, :half], x[:, :, half:]
    return jnp.concatenate([low * cos_es - high * sin_es, high * cos_es + low * sin_es], axis=2)


def solution(mesh):
    row_spec = P(("part", "dp"))
    layer_spec = P(None, "dp")

    def device_step(hidden, prompt_lens, g_attn, w_query, w_key, w_value, w_out, g_mlp, w_gate, w_up, w_down, g_final, embedding):
        batch, seq_len, dim = hidden.shape
        heads, head_dim = w_query.shape[2], w_query.shape[3]
        n_dev = dim // w_query.shape[1]
        cos_tab, sin_tab = rope_tables(seq_len, head_dim)
        cos_es, sin_es = cos_tab.T, sin_tab.T

        def headed(w):
            return w.transpose(1, 2, 0).reshape(heads * head_dim, -1)

        gains_loc = jnp.concatenate([g_attn, g_mlp, g_final[None]], axis=0)
        w_a = jnp.concatenate([headed(w_query[0]), headed(w_key[0]), headed(w_value[0]), w_out[0].T], axis=0)
        w_a = lax.all_gather(w_a, "dp", axis=1, tiled=True)
        gains = lax.all_gather(gains_loc, "dp", axis=1, tiled=True).astype(F32)
        wg = lax.all_gather(w_gate[0], "dp", axis=0, tiled=True)
        wu = lax.all_gather(w_up[0], "dp", axis=0, tiled=True)
        wd = lax.all_gather(w_down[0], "dp", axis=0, tiled=True)
        w_b = jnp.concatenate([headed(w_key[1]), headed(w_value[1])], axis=0)
        w_b = lax.all_gather(w_b, "dp", axis=1, tiled=True)
        ga0, ga1, gm0, gm1, gf = gains[0], gains[1], gains[2], gains[3], gains[4]
        hd = heads * head_dim

        normed = rms_norm(hidden, ga0)

        def project(a, w_t):
            return jnp.einsum("kd,bsd->bks", w_t, a, preferred_element_type=F32).reshape(batch, heads, head_dim, seq_len)

        q = rope_bhes(project(normed, w_a[:hd]), cos_es, sin_es).astype(BF16)
        k0 = rope_bhes(project(normed, w_a[hd:2 * hd]), cos_es, sin_es).astype(BF16)
        v0 = project(normed, w_a[2 * hd:3 * hd]).astype(BF16)
        scores = jnp.einsum("bhes,bhet->bhst", q, k0, preferred_element_type=F32) * head_dim ** -0.5
        positions = jnp.arange(seq_len)
        in_prompt = positions[None, :] < prompt_lens[:, None]
        allowed = (positions[None, :] <= positions[:, None])[None] & in_prompt[:, None, :]
        scores = jnp.where(allowed[:, None], scores, -jnp.inf)
        exp_scores = jnp.exp(scores - jnp.max(scores, axis=-1, keepdims=True))
        probs = (exp_scores / jnp.sum(exp_scores, axis=-1, keepdims=True)).astype(BF16)
        attended = jnp.einsum("bhet,bhst->bhes", v0, probs, preferred_element_type=F32)
        attended = attended.astype(BF16).reshape(batch, hd, seq_len)
        proj = jnp.einsum("bks,dk->bsd", attended, w_a[3 * hd:], preferred_element_type=F32)
        mid = (hidden.astype(F32) + proj).astype(BF16)
        normed_mlp = rms_norm(mid, gm0)
        gate_val = jnp.einsum("bsd,df->bsf", normed_mlp, wg, preferred_element_type=F32)
        up_val = jnp.einsum("bsd,df->bsf", normed_mlp, wu, preferred_element_type=F32)
        act = (jax.nn.silu(gate_val) * up_val).astype(BF16)
        down = jnp.einsum("bsf,fd->bsd", act, wd, preferred_element_type=F32)
        h1 = (mid.astype(F32) + down).astype(BF16)

        normed1 = rms_norm(h1, ga1)
        k1 = rope_bhes(project(normed1, w_b[:hd]), cos_es, sin_es).astype(BF16)
        v1 = project(normed1, w_b[hd:]).astype(BF16)

        last = prompt_lens - 1
        x = jnp.take_along_axis(h1, last[:, None, None], axis=1)[:, 0]
        me = lax.axis_index("dp")

        def spread(rows, width):
            every = lax.all_gather(rows, "dp", axis=0, tiled=True)
            return lax.dynamic_slice_in_dim(every, me * width, width, axis=1)

        def row_parallel(rows, w_loc):
            part = jnp.dot(spread(rows, w_loc.shape[0]), w_loc, preferred_element_type=F32)
            return lax.psum_scatter(part, "dp", scatter_dimension=0, tiled=True)

        a_last = rms_norm(x, ga1)
        part = jnp.einsum("bd,kd->bk", spread(a_last, dim // n_dev), headed(w_query[1]), preferred_element_type=F32)
        q1 = lax.psum_scatter(part, "dp", scatter_dimension=0, tiled=True).reshape(batch, heads, head_dim)
        half = head_dim // 2
        cos_b, sin_b = jnp.take(cos_tab, last, axis=0)[:, None], jnp.take(sin_tab, last, axis=0)[:, None]
        low, high = q1[..., :half], q1[..., half:]
        q1 = jnp.concatenate([low * cos_b - high * sin_b, high * cos_b + low * sin_b], axis=-1).astype(BF16)
        sc1 = jnp.einsum("bhe,bhet->bht", q1, k1, preferred_element_type=F32) * head_dim ** -0.5
        sc1 = jnp.where(in_prompt[:, None], sc1, -jnp.inf)
        ex1 = jnp.exp(sc1 - jnp.max(sc1, axis=-1, keepdims=True))
        pr1 = (ex1 / jnp.sum(ex1, axis=-1, keepdims=True)).astype(BF16)
        o1 = jnp.einsum("bht,bhet->bhe", pr1, v1, preferred_element_type=F32).astype(BF16).reshape(batch, hd)
        mid1 = (x.astype(F32) + row_parallel(o1, w_out[1])).astype(BF16)
        m1 = spread(rms_norm(mid1, gm1), dim // n_dev)
        ffn = w_gate.shape[2]
        parts = jnp.stack([jnp.dot(m1, w_gate[1], preferred_element_type=F32), jnp.dot(m1, w_up[1], preferred_element_type=F32)])
        sums = lax.psum_scatter(parts, "dp", scatter_dimension=2, tiled=True)
        u1 = (jax.nn.silu(sums[0]) * sums[1]).astype(BF16)
        part = jnp.dot(u1, w_down[1], preferred_element_type=F32)
        h2 = (mid1.astype(F32) + lax.psum_scatter(part, "dp", scatter_dimension=0, tiled=True)).astype(BF16)
        z = lax.all_gather(rms_norm(h2, gf), "dp", axis=0, tiled=True)
        logits = jnp.einsum("bd,vd->bv", z, embedding, preferred_element_type=F32)
        logits = lax.all_to_all(logits, "dp", split_axis=0, concat_axis=1, tiled=True)

        def cache(first, second):
            return jnp.stack([first, second]).transpose(0, 1, 4, 2, 3)

        return cache(k0, k1), cache(v0, v1), logits

    cache_spec = P(None, ("part", "dp"))
    return jax.shard_map(
        device_step,
        mesh=mesh,
        in_specs=(row_spec, row_spec) + (layer_spec,) * 9 + (P("dp"), P("dp")),
        out_specs=(cache_spec, cache_spec, row_spec),
        check_vma=False,
    )
```

```python
import functools
import math
import jax
import jax.numpy as jnp
from jax import lax
from jax.experimental import pallas as pl
from jax.experimental.pallas import tpu as pltpu
from jax.sharding import PartitionSpec as P

F32 = jnp.float32
BF16 = jnp.bfloat16
ANY = pl.BlockSpec(memory_space=pl.ANY)
VM = pl.BlockSpec(memory_space=pltpu.VMEM)
NT = (((1,), (1,)), ((), ()))


def dot(a, b):
    return jnp.dot(a, b, preferred_element_type=F32)


def dot_nt(a, b):
    return lax.dot_general(a, b, NT, preferred_element_type=F32)


def rope_tables(seq_len, head_dim):
    half_dim = head_dim // 2
    exponent = jnp.arange(half_dim, dtype=jnp.float32) * (2.0 / head_dim)
    inv_freq = 1.0 / (500000.0 ** exponent)
    wave_len = 2.0 * math.pi / inv_freq
    smooth = (8192.0 / wave_len - 1.0) / 3.0
    blended = (1.0 - smooth) * inv_freq / 8.0 + smooth * inv_freq
    scaled = jnp.where(wave_len > 8192.0, inv_freq / 8.0, jnp.where(wave_len < 2048.0, inv_freq, blended))
    angles = jnp.arange(seq_len, dtype=jnp.float32)[:, None] * scaled[None, :]
    return jnp.cos(angles), jnp.sin(angles)


def rms_norm(values, gain_f32):
    values_f32 = values.astype(F32)
    mean_sq = jnp.mean(values_f32 * values_f32, axis=-1, keepdims=True)
    return (values_f32 * lax.rsqrt(mean_sq + 1e-5) * gain_f32).astype(BF16)


ROWS = 512


def proj_body(rope, head_dim, w_ref, a_ref, cos_ref, sin_ref, *rest):
    out_ref = rest[-1]
    y = dot_nt(w_ref[...], a_ref[pl.program_id(1)])
    if not rope:
        out_ref[0, 0] = y.astype(BF16)
        return
    half = head_dim // 2
    cos, sin = cos_ref[...], sin_ref[...]
    for i in range(y.shape[0] // head_dim):
        low = y[i * head_dim:i * head_dim + half]
        high = y[i * head_dim + half:(i + 1) * head_dim]
        out_ref[0, 0, pl.ds(i * head_dim, half)] = (low * cos - high * sin).astype(BF16)
        out_ref[0, 0, pl.ds(i * head_dim + half, half)] = (high * cos + low * sin).astype(BF16)


def project(a, w, first, width, cos, sin, head_dim, rope, layers, layer, prev=None):
    b, s, d = a.shape
    grid = (width // ROWS, b)
    in_specs = [
        pl.BlockSpec((ROWS, d), lambda i, j: (first // ROWS + i, 0)),
        pl.BlockSpec((b, s, d), lambda i, j: (0, 0, 0)),
        pl.BlockSpec(cos.shape, lambda i, j: (0, 0)),
        pl.BlockSpec(sin.shape, lambda i, j: (0, 0)),
    ]
    args = [w, a, cos, sin]
    alias = {}
    if prev is not None:
        in_specs.append(ANY)
        args.append(prev)
        alias = {4: 0}
    return pl.pallas_call(
        functools.partial(proj_body, rope, head_dim),
        out_shape=jax.ShapeDtypeStruct((layers, b, width, s), BF16),
        grid=grid,
        in_specs=in_specs,
        out_specs=pl.BlockSpec((1, 1, ROWS, s), lambda i, j: (layer, j, i, 0)),
        input_output_aliases=alias,
        compiler_params=pltpu.CompilerParams(vmem_limit_bytes=40 << 20),
        cost_estimate=pl.CostEstimate(flops=2 * b * s * d * width, bytes_accessed=2 * (width * d + b * s * d + b * s * width), transcendentals=0),
        name="project",
    )(*args)


HEADS_STEP = 8


def attn_body(head_dim, lens_ref, q_ref, k_ref, v_ref, o_ref):
    s = q_ref.shape[-1]
    length = lens_ref[pl.program_id(0)]
    t_pos = lax.broadcasted_iota(jnp.int32, (s, s), 0)
    s_pos = lax.broadcasted_iota(jnp.int32, (s, s), 1)
    allowed = (t_pos <= s_pos) & (t_pos < length)
    for i in range(HEADS_STEP):
        rows = pl.ds(i * head_dim, head_dim)
        sc = lax.dot_general(k_ref[0, 0, rows], q_ref[0, 0, rows], (((0,), (0,)), ((), ())), preferred_element_type=F32)
        sc = jnp.where(allowed, sc * head_dim ** -0.5, -jnp.inf)
        ex = jnp.exp(sc - jnp.max(sc, axis=0, keepdims=True))
        p = (ex * (1.0 / jnp.sum(ex, axis=0, keepdims=True))).astype(BF16)
        o_ref[0, rows] = dot(v_ref[0, 0, rows], p).astype(BF16)


def attention(lens, q, k, v, head_dim):
    _, b, width, s = q.shape
    step = HEADS_STEP * head_dim
    spec = pl.BlockSpec((1, 1, step, s), lambda i, j, lens: (0, i, j, 0))
    return pl.pallas_call(
        functools.partial(attn_body, head_dim),
        out_shape=jax.ShapeDtypeStruct((b, width, s), BF16),
        grid_spec=pltpu.PrefetchScalarGridSpec(
            num_scalar_prefetch=1,
            grid=(b, width // step),
            in_specs=[spec, spec, spec],
            out_specs=pl.BlockSpec((1, step, s), lambda i, j, lens: (i, j, 0)),
        ),
        compiler_params=pltpu.CompilerParams(vmem_limit_bytes=40 << 20),
        cost_estimate=pl.CostEstimate(flops=4 * b * s * s * width * 8, bytes_accessed=8 * b * s * width, transcendentals=b * s * s * width // head_dim),
        name="attention",
    )(lens, q, k, v)


def last_body(head_dim, lens_ref, q_ref, k_ref, v_ref, o_ref):
    length = lens_ref[pl.program_id(0)]
    sc = dot(q_ref[0], k_ref[0, 0]) * head_dim ** -0.5
    t_pos = lax.broadcasted_iota(jnp.int32, sc.shape, 1)
    sc = jnp.where(t_pos < length, sc, -jnp.inf)
    ex = jnp.exp(sc - jnp.max(sc, axis=-1, keepdims=True))
    p = (ex / jnp.sum(ex, axis=-1, keepdims=True)).astype(BF16)
    full = dot_nt(p, v_ref[0, 0])
    head = lax.broadcasted_iota(jnp.int32, full.shape, 0)
    col = lax.broadcasted_iota(jnp.int32, full.shape, 1)
    own = (col >= head * head_dim) & (col < (head + 1) * head_dim)
    o = jnp.sum(jnp.where(own, full, 0.0), axis=0, keepdims=True)
    o_ref[0] = o.astype(BF16).astype(F32)


def last_attention(lens, q_diag, k, v, head_dim, layer):
    b, heads, width = q_diag.shape
    s = k.shape[-1]
    kv = pl.BlockSpec((1, 1, width, s), lambda i, lens: (layer, i, 0, 0))
    return pl.pallas_call(
        functools.partial(last_body, head_dim),
        out_shape=jax.ShapeDtypeStruct((b, 1, width), F32),
        grid_spec=pltpu.PrefetchScalarGridSpec(
            num_scalar_prefetch=1,
            grid=(b,),
            in_specs=[pl.BlockSpec((1, heads, width), lambda i, lens: (i, 0, 0)), kv, kv],
            out_specs=pl.BlockSpec((1, 1, width), lambda i, lens: (i, 0, 0)),
        ),
        compiler_params=pltpu.CompilerParams(vmem_limit_bytes=40 << 20),
        cost_estimate=pl.CostEstimate(flops=4 * b * s * width * heads, bytes_accessed=4 * b * s * width, transcendentals=b * s * heads),
        name="last_attention",
    )(lens, q_diag, k, v)[:, 0]


class Exchange:
    def __init__(self, n, send_sems, recv_sems):
        self.n, self.send_sems, self.recv_sems = n, send_sems, recv_sems
        self.me = lax.axis_index("dp")

    def peer(self, j):
        return lax.rem(self.me + j, self.n)

    def barrier(self):
        sem = pltpu.get_barrier_semaphore()
        for j in range(1, self.n):
            pl.semaphore_signal(sem, inc=1, device_id={"dp": self.peer(j)}, device_id_type=pl.DeviceIdType.MESH)
        pl.semaphore_wait(sem, self.n - 1)

    def copy(self, stage, j, src, dst):
        return pltpu.make_async_remote_copy(
            src_ref=src, dst_ref=dst, send_sem=self.send_sems.at[stage, j], recv_sem=self.recv_sems.at[stage, self.me],
            device_id={"dp": self.peer(j)}, device_id_type=pl.DeviceIdType.MESH)

    def arrival(self, stage, j, src, dst):
        return pltpu.make_async_remote_copy(
            src_ref=src, dst_ref=dst, send_sem=self.send_sems.at[stage, j], recv_sem=self.recv_sems.at[stage, self.peer(j)],
            device_id={"dp": self.peer(j)}, device_id_type=pl.DeviceIdType.MESH)

    def start(self, stage, src_of, dst):
        for j in range(1, self.n):
            self.copy(stage, j, src_of(j), dst).start()

    def wait(self, stage, src_of, dst_from):
        for j in range(1, self.n):
            self.arrival(stage, j, src_of(j), dst_from(self.peer(j))).wait_recv()
        for j in range(1, self.n):
            self.arrival(stage, j, src_of(j), dst_from(self.peer(j))).wait_send()


def columns(ref, index, width):
    return ref.at[:, pl.ds(pl.multiple_of(index * width, width), width)]


def spread(ex, stage, rows_ref, got_ref, lhs_ref):
    n, rows, width = got_ref.shape
    src = lambda j: columns(rows_ref, ex.peer(j), width)
    ex.start(stage, src, got_ref.at[ex.me])
    got_ref[ex.me] = columns(rows_ref, ex.me, width)[...]
    ex.wait(stage, src, lambda p: got_ref.at[p])
    for i in range(n):
        lhs_ref[pl.ds(i * rows, rows)] = got_ref[i]
    return lhs_ref[...].astype(BF16)


def reduce_rows(ex, stage, part, send_ref, got_ref):
    n, rows, _ = got_ref.shape
    for i in range(n):
        send_ref[i] = part[i * rows:(i + 1) * rows]
    src = lambda j: send_ref.at[ex.peer(j)]
    ex.start(stage, src, got_ref.at[ex.me])
    got_ref[ex.me] = send_ref[ex.me]
    ex.wait(stage, src, lambda p: got_ref.at[p])
    total = got_ref[0]
    for i in range(1, n):
        total = total + got_ref[i]
    return total


def query_body(n, a_ref, w_ref, q_ref, got, lhs, send, back, send_sems, recv_sems):
    ex = Exchange(n, send_sems, recv_sems)
    ex.barrier()
    x = spread(ex, 0, a_ref, got, lhs)
    q_ref[...] = reduce_rows(ex, 1, dot_nt(x, w_ref[...]), send, back)


def last_query(a_last, w_rows, n):
    rows, d = a_last.shape
    width, kd = w_rows.shape
    return pl.pallas_call(
        functools.partial(query_body, n),
        out_shape=jax.ShapeDtypeStruct((rows, width), F32),
        in_specs=[VM, VM],
        out_specs=VM,
        scratch_shapes=[
            pltpu.VMEM((n, rows, kd), F32), pltpu.VMEM((n * rows, kd), F32),
            pltpu.VMEM((n, rows, width), F32), pltpu.VMEM((n, rows, width), F32),
            pltpu.SemaphoreType.DMA((2, n)), pltpu.SemaphoreType.DMA((2, n)),
        ],
        compiler_params=pltpu.CompilerParams(collective_id=0, has_side_effects=True, vmem_limit_bytes=16 << 20),
        cost_estimate=pl.CostEstimate(flops=2 * n * rows * width * kd, bytes_accessed=2 * width * kd, transcendentals=0),
        name="last_query",
    )(a_last, w_rows)


GROUPS = 3
TABLE_STEP = 512


def tail_body(n, layer, o_ref, x_ref, gm_ref, gf_ref, wo_hbm, wg_hbm, wu_hbm, wd_hbm, emb_hbm, out_ref,
              wo, wg, wu, wd, emb, got, lhs, send, back, mid_ref, rows_ref, gate_send, gate_got, z_got, z_lhs,
              log_send, log_got, local_sems, send_sems, recv_sems):
    ex = Exchange(n, send_sems, recv_sems)
    me = ex.me
    loads = [
        pltpu.make_async_copy(wo_hbm.at[layer], wo, local_sems.at[0]),
        pltpu.make_async_copy(wg_hbm.at[layer], wg, local_sems.at[1]),
        pltpu.make_async_copy(wu_hbm.at[layer], wu, local_sems.at[2]),
        pltpu.make_async_copy(wd_hbm.at[layer], wd, local_sems.at[3]),
        pltpu.make_async_copy(emb_hbm, emb, local_sems.at[4]),
    ]
    for load in loads:
        load.start()
    ex.barrier()

    x = spread(ex, 0, o_ref, got, lhs)
    loads[0].wait()
    mid = (x_ref[...] + reduce_rows(ex, 1, dot(x, wo[...]), send, back)).astype(BF16).astype(F32)
    mid_ref[...] = mid

    rows_ref[...] = rms_norm(mid, gm_ref[...]).astype(F32)
    x = spread(ex, 2, rows_ref, got, lhs)
    loads[1].wait()
    loads[2].wait()
    block = wd.shape[0]

    def gate_up(p):
        cols = pl.ds(pl.multiple_of(p * block, block), block)
        return dot(x, wg[:, cols]), dot(x, wu[:, cols])

    for j in range(1, n):
        gate, up = gate_up(ex.peer(j))
        gate_send[j, 0] = gate
        gate_send[j, 1] = up
        ex.copy(3, j, gate_send.at[j], gate_got.at[me]).start()
    gate, up = gate_up(me)
    gate_got[me, 0] = gate
    gate_got[me, 1] = up
    ex.wait(3, lambda j: gate_send.at[j], lambda p: gate_got.at[p])
    gate, up = gate_got[0, 0], gate_got[0, 1]
    for i in range(1, n):
        gate = gate + gate_got[i, 0]
        up = up + gate_got[i, 1]
    act = (gate * (1.0 / (1.0 + jnp.exp(-gate))) * up).astype(BF16)

    loads[3].wait()
    h = (mid_ref[...] + reduce_rows(ex, 4, dot(act, wd[...]), send, back)).astype(BF16).astype(F32)

    rows_ref[...] = rms_norm(h, gf_ref[...]).astype(F32)
    rows = rows_ref.shape[0]
    ex.start(5, lambda j: rows_ref, z_got.at[me])
    z_got[me] = rows_ref[...]
    ex.wait(5, lambda j: rows_ref, lambda p: z_got.at[p])
    for i in range(n):
        z_lhs[pl.ds(i * rows, rows)] = z_got[i]
    z = z_lhs[...].astype(BF16)
    loads[4].wait()
    vocab = emb.shape[0]
    group = vocab // GROUPS
    for g in range(GROUPS):
        def step(c, carry):
            first = pl.multiple_of(g * group + c * TABLE_STEP, TABLE_STEP)
            part = dot_nt(z, emb[pl.ds(first, TABLE_STEP)])
            for i in range(n):
                log_send[i, :, pl.ds(first, TABLE_STEP)] = part[i * rows:(i + 1) * rows]
            return carry

        lax.fori_loop(0, group // TABLE_STEP, step, 0)
        src = lambda j, g=g: log_send.at[ex.peer(j), :, pl.ds(g * group, group)]
        dst = lambda p, g=g: log_got.at[:, pl.ds(pl.multiple_of(p * vocab + g * group, group), group)]
        ex.start(6 + g, src, dst(me))
    log_got[:, pl.ds(pl.multiple_of(me * vocab, vocab), vocab)] = log_send[me]
    for g in range(GROUPS):
        src = lambda j, g=g: log_send.at[ex.peer(j), :, pl.ds(g * group, group)]
        dst = lambda p, g=g: log_got.at[:, pl.ds(pl.multiple_of(p * vocab + g * group, group), group)]
        ex.wait(6 + g, src, dst)
    out_ref[...] = log_got[...]


def tail(o, x, gm, gf, w_out, w_gate, w_up, w_down, emb, layer, n):
    rows, d = x.shape
    kd, ffn, block, vocab = w_gate.shape[1], w_gate.shape[2], w_down.shape[1], emb.shape[0]
    stages = 6 + GROUPS
    flops = 2 * n * rows * (kd * d + 2 * kd * ffn + block * d + vocab * d)
    return pl.pallas_call(
        functools.partial(tail_body, n, layer),
        out_shape=jax.ShapeDtypeStruct((rows, n * vocab), F32),
        in_specs=[VM, VM, VM, VM] + [ANY] * 5,
        out_specs=VM,
        scratch_shapes=[
            pltpu.VMEM((kd, d), BF16), pltpu.VMEM((kd, ffn), BF16), pltpu.VMEM((kd, ffn), BF16),
            pltpu.VMEM((block, d), BF16), pltpu.VMEM((vocab, d), BF16),
            pltpu.VMEM((n, rows, kd), F32), pltpu.VMEM((n * rows, kd), F32),
            pltpu.VMEM((n, rows, d), F32), pltpu.VMEM((n, rows, d), F32),
            pltpu.VMEM((rows, d), F32), pltpu.VMEM((rows, d), F32),
            pltpu.VMEM((n, 2, n * rows, block), F32), pltpu.VMEM((n, 2, n * rows, block), F32),
            pltpu.VMEM((n, rows, d), F32), pltpu.VMEM((n * rows, d), F32),
            pltpu.VMEM((n, rows, vocab), F32), pltpu.VMEM((rows, n * vocab), F32),
            pltpu.SemaphoreType.DMA((5,)), pltpu.SemaphoreType.DMA((stages, n)), pltpu.SemaphoreType.DMA((stages, n)),
        ],
        compiler_params=pltpu.CompilerParams(collective_id=1, has_side_effects=True, vmem_limit_bytes=58 << 20),
        cost_estimate=pl.CostEstimate(flops=flops, bytes_accessed=flops // (n * rows), transcendentals=0),
        name="tail",
    )(o, x, gm, gf, w_out, w_gate, w_up, w_down, emb)


def solution(mesh):
    row_spec = P(("part", "dp"))
    layer_spec = P(None, "dp")

    def device_step(hidden, prompt_lens, g_attn, w_query, w_key, w_value, w_out, g_mlp, w_gate, w_up, w_down, g_final, embedding):
        batch, seq_len, dim = hidden.shape
        heads, head_dim = w_query.shape[2], w_query.shape[3]
        n_dev = dim // w_query.shape[1]
        cos_tab, sin_tab = rope_tables(seq_len, head_dim)
        cos_es, sin_es = cos_tab.T, sin_tab.T

        def headed(w):
            return w.transpose(1, 2, 0).reshape(heads * head_dim, -1)

        gains_loc = jnp.concatenate([g_attn, g_mlp, g_final[None]], axis=0)
        w_a = jnp.concatenate([headed(w_query[0]), headed(w_key[0]), headed(w_value[0]), w_out[0].T], axis=0)
        w_a = lax.all_gather(w_a, "dp", axis=1, tiled=True)
        gains = lax.all_gather(gains_loc, "dp", axis=1, tiled=True).astype(F32)
        wg = lax.all_gather(w_gate[0], "dp", axis=0, tiled=True)
        wu = lax.all_gather(w_up[0], "dp", axis=0, tiled=True)
        wd = lax.all_gather(w_down[0], "dp", axis=0, tiled=True)
        w_b = jnp.concatenate([headed(w_key[1]), headed(w_value[1])], axis=0)
        w_b = lax.all_gather(w_b, "dp", axis=1, tiled=True)
        ga0, ga1, gm0, gm1, gf = gains[0], gains[1], gains[2], gains[3], gains[4]
        hd = heads * head_dim

        lens = prompt_lens
        rope = (cos_es, sin_es, head_dim)
        normed = rms_norm(hidden, ga0)
        q0 = project(normed, w_a, 0, hd, *rope, True, 1, 0)
        k_cache = project(normed, w_a, hd, hd, *rope, True, 2, 0)
        v_cache = project(normed, w_a, 2 * hd, hd, *rope, False, 2, 0)
        attended = attention(lens, q0, k_cache, v_cache, head_dim)
        proj = jnp.einsum("bks,dk->bsd", attended, w_a[3 * hd:], preferred_element_type=F32)
        mid = (hidden.astype(F32) + proj).astype(BF16)
        normed_mlp = rms_norm(mid, gm0)
        gate_val = jnp.einsum("bsd,df->bsf", normed_mlp, wg, preferred_element_type=F32)
        up_val = jnp.einsum("bsd,df->bsf", normed_mlp, wu, preferred_element_type=F32)
        act = (jax.nn.silu(gate_val) * up_val).astype(BF16)
        down = jnp.einsum("bsf,fd->bsd", act, wd, preferred_element_type=F32)
        h1 = (mid.astype(F32) + down).astype(BF16)

        last = lens - 1
        x = jnp.take_along_axis(h1, last[:, None, None], axis=1)[:, 0]
        q1 = last_query(rms_norm(x, ga1).astype(F32), headed(w_query[1]), n_dev).reshape(batch, heads, head_dim)
        half = head_dim // 2
        cos_b, sin_b = jnp.take(cos_tab, last, axis=0)[:, None], jnp.take(sin_tab, last, axis=0)[:, None]
        low, high = q1[..., :half], q1[..., half:]
        q1 = jnp.concatenate([low * cos_b - high * sin_b, high * cos_b + low * sin_b], axis=-1).astype(BF16)
        own = jnp.arange(hd)[None, :] // head_dim == jnp.arange(heads)[:, None]
        q_diag = jnp.where(own[None], q1.reshape(batch, 1, hd), jnp.zeros((), BF16))

        normed1 = rms_norm(h1, ga1)
        k_cache = project(normed1, w_b, 0, hd, *rope, True, 2, 1, k_cache)
        v_cache = project(normed1, w_b, hd, hd, *rope, False, 2, 1, v_cache)

        o1 = last_attention(lens, q_diag, k_cache, v_cache, head_dim, 1)
        logits = tail(o1, x.astype(F32), gm1[None], gf[None], w_out, w_gate, w_up, w_down, embedding, 1, n_dev)

        def cache(c):
            return c.reshape(2, batch, heads, head_dim, seq_len).transpose(0, 1, 4, 2, 3)

        return cache(k_cache), cache(v_cache), logits

    cache_spec = P(None, ("part", "dp"))
    return jax.shard_map(
        device_step,
        mesh=mesh,
        in_specs=(row_spec, row_spec) + (layer_spec,) * 9 + (P("dp"), P("dp")),
        out_specs=(cache_spec, cache_spec, row_spec),
        check_vma=False,
    )
```

```python
import functools
import math
import jax
import jax.numpy as jnp
import numpy as np
from jax import lax
from jax.experimental import pallas as pl
from jax.experimental.pallas import tpu as pltpu
from jax.sharding import PartitionSpec as P

F32 = jnp.float32
BF16 = jnp.bfloat16
ANY = pl.BlockSpec(memory_space=pl.ANY)
HBM = pl.BlockSpec(memory_space=pltpu.HBM)
VM = pl.BlockSpec(memory_space=pltpu.VMEM)
NT = (((1,), (1,)), ((), ()))


def params(mib, collective=None):
    extra = {} if collective is None else dict(collective_id=collective, has_side_effects=True)
    return pltpu.CompilerParams(vmem_limit_bytes=mib << 20, **extra)


def cost(macs, values, exps=0):
    return pl.CostEstimate(flops=2 * macs, bytes_accessed=2 * values, transcendentals=exps)


def dot(a, b):
    return jnp.dot(a, b, preferred_element_type=F32)


def dot_nt(a, b):
    return lax.dot_general(a, b, NT, preferred_element_type=F32)


def rope_frequencies(head_dim):
    half_dim = head_dim // 2
    exponent = np.arange(half_dim, dtype=np.float32) * np.float32(2.0 / head_dim)
    inv_freq = np.float32(1.0) / np.float32(500000.0) ** exponent
    wave_len = np.float32(2.0 * math.pi) / inv_freq
    smooth = (np.float32(8192.0) / wave_len - np.float32(1.0)) / np.float32(3.0)
    blended = (1 - smooth) * inv_freq / 8 + smooth * inv_freq
    scaled = np.where(wave_len > 8192.0, inv_freq / 8, np.where(wave_len < 2048.0, inv_freq, blended))
    return scaled.astype(np.float32)


def rms_norm(values, gain_f32):
    values_f32 = values.astype(F32)
    mean_sq = jnp.mean(values_f32 * values_f32, axis=-1, keepdims=True)
    return (values_f32 * lax.rsqrt(mean_sq + 1e-5) * gain_f32).astype(BF16)


ROWS = 1024
PAIR = 2


def proj_body(ropes, per, head_dim, n_prev, norm, w_ref, a_ref, cos_ref, sin_ref, *rest):
    s = cos_ref.shape[1]
    half = head_dim // 2
    if norm:
        gain_ref, a_src, a_ref = rest[0], a_ref, rest[-1]
        rest = rest[1:-1]

        @pl.when((pl.program_id(0) == 0) & (pl.program_id(1) == 0))
        def _():
            normalize(a_src, gain_ref, a_ref)

    outs = rest[n_prev:]
    first = pl.multiple_of(pl.program_id(1) * PAIR * s, PAIR * s)
    y = dot_nt(w_ref[...], a_ref[pl.ds(first, PAIR * s)])

    def store(rope, out_ref):
        for t in range(PAIR):
            part = y[:, t * s:(t + 1) * s]
            if not rope:
                out_ref[0, t] = part.astype(BF16)
                continue
            cos, sin = cos_ref[...], sin_ref[...]
            for i in range(ROWS // head_dim):
                low = part[i * head_dim:i * head_dim + half]
                high = part[i * head_dim + half:(i + 1) * head_dim]
                out_ref[0, t, pl.ds(i * head_dim, half)] = (low * cos - high * sin).astype(BF16)
                out_ref[0, t, pl.ds(i * head_dim + half, half)] = (high * cos + low * sin).astype(BF16)

    for k, (rope, out_ref) in enumerate(zip(ropes, outs)):
        pl.when(pl.program_id(0) // per == k)(functools.partial(store, rope, out_ref))


def project(a, w, cos, sin, head_dim, ropes, layers, layer, prev=None, gain=None):
    rows, d = a.shape
    s = cos.shape[1]
    b, width = rows // s, w.shape[0] // len(ropes)
    per = width // ROWS
    last = b // PAIR - 1

    def place(k):
        def index(i, j):
            at = i - k * per
            inside = (at >= 0) & (at < per)
            return layer, jnp.where(inside, j, jnp.where(at < 0, 0, last)), jnp.clip(at, 0, per - 1), 0
        return pl.BlockSpec((1, PAIR, ROWS, s), index)

    in_specs = [
        pl.BlockSpec((ROWS, d), lambda i, j: (i, 0)),
        pl.BlockSpec((rows, d), lambda i, j: (0, 0)),
        pl.BlockSpec(cos.shape, lambda i, j: (0, 0)),
        pl.BlockSpec(sin.shape, lambda i, j: (0, 0)),
    ]
    args = [w, a, cos, sin]
    alias = {}
    out_shape = [jax.ShapeDtypeStruct((count, b, width, s), BF16) for count in layers]
    out_specs = [place(k) for k in range(len(ropes))]
    if gain is not None:
        in_specs.append(pl.BlockSpec(gain.shape, lambda i, j: (0, 0)))
        args.append(gain)
        out_shape.append(jax.ShapeDtypeStruct(a.shape, BF16))
        out_specs.append(pl.BlockSpec(a.shape, lambda i, j: (0, 0)))
    if prev is not None:
        alias = {len(args): 0}
        in_specs.append(HBM)
        args.append(prev)
    return pl.pallas_call(
        functools.partial(proj_body, ropes, per, head_dim, len(alias), gain is not None),
        out_shape=out_shape,
        grid=(w.shape[0] // ROWS, b // PAIR),
        in_specs=in_specs,
        out_specs=out_specs,
        input_output_aliases=alias,
        compiler_params=params(58),
        cost_estimate=cost(rows * d * w.shape[0], w.size + a.size + a.size),
        name="project",
    )(*args)


TILE = 512
BAND = 1024


def normalize(src_ref, gain_ref, dst_ref):
    lines = 32

    def step(r, carry):
        rows = pl.ds(pl.multiple_of(r * lines, lines), lines)
        dst_ref[rows] = rms_norm(src_ref[rows], gain_ref[...])
        return carry

    lax.fori_loop(0, src_ref.shape[0] // lines, step, 0, unroll=4)


def gate_up_tile(x, wg_ref, wu_ref, o_ref):
    gate = dot(x, wg_ref[...])
    up = dot(x, wu_ref[...])
    o_ref[...] = (gate * (1.0 / (1.0 + jnp.exp(-gate))) * up).astype(BF16)


def gate_up_first_body(h_ref, gain_ref, wg_ref, wu_ref, o_ref, m_ref):
    @pl.when((pl.program_id(0) == 0) & (pl.program_id(1) == 0))
    def _():
        normalize(h_ref, gain_ref, m_ref)

    gate_up_tile(m_ref[pl.ds(pl.multiple_of(pl.program_id(1) * BAND, BAND), BAND)], wg_ref, wu_ref, o_ref)


def gate_up_rest_body(m_ref, wg_ref, wu_ref, o_ref):
    gate_up_tile(m_ref[pl.ds(pl.multiple_of(pl.program_id(1) * BAND, BAND), BAND)], wg_ref, wu_ref, o_ref)


def gate_up(rows_in, gain, weights, width):
    rows, d = rows_in.shape
    whole = pl.BlockSpec((rows, d), lambda i, j: (0, 0))
    out_shape = [jax.ShapeDtypeStruct((rows, width), BF16)]
    out_specs = [pl.BlockSpec((BAND, TILE), lambda i, j: (j, i))]
    if gain is not None:
        body, lead, args = gate_up_first_body, [whole, pl.BlockSpec(gain.shape, lambda i, j: (0, 0))], (rows_in, gain) + weights
        specs = [pl.BlockSpec((d, TILE), lambda i, j: (0, i))] * 2
        out_shape.append(jax.ShapeDtypeStruct((rows, d), BF16))
        out_specs.append(whole)
    else:
        body, lead, args = gate_up_rest_body, [whole], (rows_in,) + weights * 2
        specs = [pl.BlockSpec((None, d, TILE), lambda i, j, k=k: (k, 0, i)) for k in range(2)]
    return pl.pallas_call(
        body,
        out_shape=out_shape,
        grid=(width // TILE, rows // BAND),
        in_specs=lead + specs,
        out_specs=out_specs,
        compiler_params=params(60),
        cost_estimate=cost(2 * rows * d * width, 2 * d * width + rows * (d + width), rows * width),
        name="gate_up",
    )(*args)


def down_body(has_base, a_ref, w_ref, *rest):
    y = dot(a_ref[...], w_ref[...])
    if has_base:
        base_ref, part_ref, o_ref = rest
        o_ref[...] = (base_ref[...].astype(F32) + (part_ref[...] + y)).astype(BF16)
    else:
        rest[0][...] = y


def down(act, w, band, base=None):
    rows, kd = act.shape
    d = w.shape[1]
    tile = pl.BlockSpec((band, TILE), lambda i, j: (i, j))
    base = base or ()
    return pl.pallas_call(
        functools.partial(down_body, bool(base)),
        out_shape=jax.ShapeDtypeStruct((rows, d), BF16 if base else F32),
        grid=(rows // band, d // TILE),
        in_specs=[pl.BlockSpec((band, kd), lambda i, j: (i, 0)), pl.BlockSpec((kd, TILE), lambda i, j: (0, j))] + [tile] * len(base),
        out_specs=tile,
        compiler_params=params(60),
        cost_estimate=cost(rows * d * kd, rows * kd + kd * d + 3 * rows * d),
        name="down",
    )(act, w, *base)


HEADS_STEP = 8


def attn_body(head_dim, lens_ref, q_ref, k_ref, v_ref, o_ref):
    s = q_ref.shape[-1]
    length = lens_ref[pl.program_id(0)]
    t_pos = lax.broadcasted_iota(jnp.int32, (s, s), 0)
    s_pos = lax.broadcasted_iota(jnp.int32, (s, s), 1)
    allowed = (t_pos <= s_pos) & (t_pos < length)
    for i in range(HEADS_STEP):
        rows = pl.ds(i * head_dim, head_dim)
        q = q_ref[0, 0, rows] * jnp.asarray(head_dim ** -0.5, BF16)
        sc = lax.dot_general(k_ref[0, 0, rows], q, (((0,), (0,)), ((), ())), preferred_element_type=F32)
        sc = jnp.where(allowed, sc, -jnp.inf)
        ex = jnp.exp(sc - jnp.max(sc, axis=0, keepdims=True))
        p = (ex * (1.0 / jnp.sum(ex, axis=0, keepdims=True))).astype(BF16)
        o_ref[0, rows] = dot(v_ref[0, 0, rows], p).astype(BF16)


def attention(lens, q, k, v, head_dim):
    _, b, width, s = q.shape
    step = HEADS_STEP * head_dim
    spec = pl.BlockSpec((1, 1, step, s), lambda i, j, lens: (0, i, j, 0))
    return pl.pallas_call(
        functools.partial(attn_body, head_dim),
        out_shape=jax.ShapeDtypeStruct((b, width, s), BF16),
        grid_spec=pltpu.PrefetchScalarGridSpec(
            num_scalar_prefetch=1,
            grid=(b, width // step),
            in_specs=[spec, spec, spec],
            out_specs=pl.BlockSpec((1, step, s), lambda i, j, lens: (i, j, 0)),
        ),
        compiler_params=params(40),
        cost_estimate=cost(16 * b * s * s * width, 4 * b * s * width, b * s * s * width // head_dim),
        name="attention",
    )(lens, q, k, v)


def last_body(head_dim, lens_ref, q_ref, k_ref, v_ref, o_ref):
    length = lens_ref[pl.program_id(0)]
    sc = dot(q_ref[0], k_ref[0, 0]) * head_dim ** -0.5
    t_pos = lax.broadcasted_iota(jnp.int32, sc.shape, 1)
    sc = jnp.where(t_pos < length, sc, -jnp.inf)
    ex = jnp.exp(sc - jnp.max(sc, axis=-1, keepdims=True))
    p = (ex / jnp.sum(ex, axis=-1, keepdims=True)).astype(BF16)
    full = dot_nt(p, v_ref[0, 0])
    head = lax.broadcasted_iota(jnp.int32, full.shape, 0)
    col = lax.broadcasted_iota(jnp.int32, full.shape, 1)
    own = (col >= head * head_dim) & (col < (head + 1) * head_dim)
    o = jnp.sum(jnp.where(own, full, 0.0), axis=0, keepdims=True)
    o_ref[0] = o.astype(BF16).astype(F32)


def last_attention(lens, q_diag, k, v, head_dim, layer):
    b, heads, width = q_diag.shape
    s = k.shape[-1]
    kv = pl.BlockSpec((1, 1, width, s), lambda i, lens: (layer, i, 0, 0))
    return pl.pallas_call(
        functools.partial(last_body, head_dim),
        out_shape=jax.ShapeDtypeStruct((b, 1, width), F32),
        grid_spec=pltpu.PrefetchScalarGridSpec(
            num_scalar_prefetch=1,
            grid=(b,),
            in_specs=[pl.BlockSpec((1, heads, width), lambda i, lens: (i, 0, 0)), kv, kv],
            out_specs=pl.BlockSpec((1, 1, width), lambda i, lens: (i, 0, 0)),
        ),
        compiler_params=params(40),
        cost_estimate=cost(2 * b * s * width * heads, 2 * b * s * width, b * s * heads),
        name="last_attention",
    )(lens, q_diag, k, v)[:, 0]


class Exchange:
    def __init__(self, n, send_sems, recv_sems):
        self.n, self.send_sems, self.recv_sems = n, send_sems, recv_sems
        self.me = lax.axis_index("dp")

    def peer(self, j):
        return lax.rem(self.me + j, self.n)

    def barrier(self):
        sem = pltpu.get_barrier_semaphore()
        for j in range(1, self.n):
            pl.semaphore_signal(sem, inc=1, device_id={"dp": self.peer(j)}, device_id_type=pl.DeviceIdType.MESH)
        pl.semaphore_wait(sem, self.n - 1)

    def copy(self, stage, j, src, dst):
        return pltpu.make_async_remote_copy(
            src_ref=src, dst_ref=dst, send_sem=self.send_sems.at[stage, j], recv_sem=self.recv_sems.at[stage, self.me],
            device_id={"dp": self.peer(j)}, device_id_type=pl.DeviceIdType.MESH)

    def arrival(self, stage, j, src, dst):
        return pltpu.make_async_remote_copy(
            src_ref=src, dst_ref=dst, send_sem=self.send_sems.at[stage, j], recv_sem=self.recv_sems.at[stage, self.peer(j)],
            device_id={"dp": self.peer(j)}, device_id_type=pl.DeviceIdType.MESH)

    def start(self, stage, src_of, dst):
        for j in range(1, self.n):
            self.copy(stage, j, src_of(j), dst).start()

    def wait(self, stage, src_of, dst_from):
        for j in range(1, self.n):
            self.arrival(stage, j, src_of(j), dst_from(self.peer(j))).wait_recv()
        for j in range(1, self.n):
            self.arrival(stage, j, src_of(j), dst_from(self.peer(j))).wait_send()


def columns(ref, index, width):
    return ref.at[:, pl.ds(pl.multiple_of(index * width, width), width)]


def spread(ex, stage, rows_ref, got_ref, lhs_ref):
    n, rows, width = got_ref.shape
    src = lambda j: columns(rows_ref, ex.peer(j), width)
    ex.start(stage, src, got_ref.at[ex.me])
    got_ref[ex.me] = columns(rows_ref, ex.me, width)[...]
    ex.wait(stage, src, lambda p: got_ref.at[p])
    for i in range(n):
        lhs_ref[pl.ds(i * rows, rows)] = got_ref[i]
    return lhs_ref[...].astype(BF16)


def reduce_rows(ex, stage, part, send_ref, got_ref):
    n, rows, _ = got_ref.shape
    for i in range(n):
        send_ref[i] = part[i * rows:(i + 1) * rows]
    src = lambda j: send_ref.at[ex.peer(j)]
    ex.start(stage, src, got_ref.at[ex.me])
    got_ref[ex.me] = send_ref[ex.me]
    ex.wait(stage, src, lambda p: got_ref.at[p])
    total = got_ref[0]
    for i in range(1, n):
        total = total + got_ref[i]
    return total


def query_body(n, layer, a_ref, w_hbm, q_ref, w, got, lhs, send, back, local_sem, send_sems, recv_sems):
    load = pltpu.make_async_copy(w_hbm.at[layer], w, local_sem)
    load.start()
    ex = Exchange(n, send_sems, recv_sems)
    ex.barrier()
    x = spread(ex, 0, a_ref, got, lhs)
    load.wait()
    q_ref[...] = reduce_rows(ex, 1, dot_nt(x, w[...]), send, back)


def last_query(a_last, w_rows, layer, n):
    rows, d = a_last.shape
    _, width, kd = w_rows.shape
    return pl.pallas_call(
        functools.partial(query_body, n, layer),
        out_shape=jax.ShapeDtypeStruct((rows, width), F32),
        in_specs=[VM, HBM],
        out_specs=VM,
        scratch_shapes=[
            pltpu.VMEM((width, kd), BF16),
            pltpu.VMEM((n, rows, kd), F32), pltpu.VMEM((n * rows, kd), F32),
            pltpu.VMEM((n, rows, width), F32), pltpu.VMEM((n, rows, width), F32),
            pltpu.SemaphoreType.DMA, pltpu.SemaphoreType.DMA((2, n)), pltpu.SemaphoreType.DMA((2, n)),
        ],
        compiler_params=params(16, 0),
        cost_estimate=cost(n * rows * width * kd, width * kd),
        name="last_query",
    )(a_last, w_rows)


class Place:
    def __init__(self):
        me = lax.axis_index("dp")
        core, col, row = lax.rem(me, 2), lax.rem(me // 2, 2), me // 4
        at = lambda r, c, k: r * 4 + c * 2 + k
        self.me = me
        self.sib = at(row, col, 1 - core)
        self.xn, self.yn, self.dg = at(row, 1 - col, core), at(1 - row, col, core), at(1 - row, 1 - col, core)
        self.xs, self.ys, self.ds = at(row, 1 - col, 1 - core), at(1 - row, col, 1 - core), at(1 - row, 1 - col, 1 - core)


def remote(src, dst, send_sem, recv_sem, dev):
    return pltpu.make_async_remote_copy(src_ref=src, dst_ref=dst, send_sem=send_sem, recv_sem=recv_sem,
                                        device_id={"dp": dev}, device_id_type=pl.DeviceIdType.MESH)


def greet(devs):
    sem = pltpu.get_barrier_semaphore()
    for dev in devs:
        pl.semaphore_signal(sem, inc=1, device_id={"dp": dev}, device_id_type=pl.DeviceIdType.MESH)
    pl.semaphore_wait(sem, len(devs))


def gather_body(n, plan, n_in, n_out, *refs):
    ins, outs = refs[:n_in], refs[n_in:n_in + n_out]
    (stage, keep, gain_got, gain_row, raw, normed, load_sems, pack_sems, keep_sems, gain_send, gain_recv, row_sems, own_sems,
     send_sems, recv_sems) = refs[n_in + n_out:]
    at = Place()
    me = at.me
    gain_ref, hidden = ins[:2]
    gains_out, normed_out = outs[:2]
    jobs, pack_in, pack_out = plan(ins[2:], outs[2:], stage, keep)
    count = len(jobs)
    loads, taken = [], 0
    for pieces, _, _, _ in jobs:
        loads.append([pltpu.make_async_copy(src, dst, load_sems.at[taken + i]) for i, (src, dst) in enumerate(pieces)])
        taken += len(pieces)
    for copy in sum(loads, []):
        copy.start()
    batch = hidden.shape[0]
    row_in = [pltpu.make_async_copy(hidden.at[i], raw.at[i % 2], row_sems.at[0, i]) for i in range(batch)]
    row_out = [pltpu.make_async_copy(normed.at[i % 2], normed_out.at[i], row_sems.at[1, i]) for i in range(batch)]
    pack_in = [pltpu.make_async_copy(src, dst, pack_sems.at[i]) for i, (src, dst) in enumerate(pack_in)]
    pack_out = [pltpu.make_async_copy(src, dst, keep_sems.at[i]) for i, (src, dst) in enumerate(pack_out)]
    peers = [lax.rem(me + j, n) for j in range(1, n)]
    greet(peers)

    def gain_to(j):
        return remote(gain_ref, gain_got.at[me], gain_send.at[j], gain_recv.at[me], peers[j])

    def gain_from(j):
        return remote(gain_ref, gain_got.at[peers[j]], gain_send.at[j], gain_recv.at[peers[j]], peers[j])

    def share_gains():
        for j in range(n - 1):
            gain_to(j).start()
        gain_got[me] = gain_ref[...]

    def normalize():
        for j in range(n - 1):
            gain_from(j).wait_recv()
            gain_from(j).wait_send()
        gains_out[...] = gain_got[...]
        width = gain_ref.shape[1]
        for i in range(n):
            gain_row[:, pl.ds(i * width, width)] = gain_got[i, pl.ds(0, 1)]
        block = 32
        for i in range(batch):
            row_in[i].wait()
            if i >= 2:
                row_out[i - 2].wait()

            def step(r, carry, i=i):
                rows = pl.ds(pl.multiple_of(r * block, block), block)
                normed[i % 2, rows] = rms_norm(raw[i % 2, rows], gain_row[...])
                return carry

            lax.fori_loop(0, raw.shape[1] // block, step, 0)
            row_out[i].start()
            if i + 2 < batch:
                row_in[i + 2].start()

    def hop(k, i):
        _, buf, full, half = jobs[i]
        route = (
            (buf, full(at.me), at.xn, full(at.xn)),
            (buf, full(at.me), at.yn, full(at.yn)),
            (buf, full(at.me), at.sib, full(at.sib)),
            (half(at.xn, 0), half(at.xn, 0), at.yn, half(at.dg, 0)),
            (half(at.yn, 1), half(at.yn, 1), at.xn, half(at.dg, 1)),
            (full(at.xn), full(at.xn), at.sib, full(at.xs)),
            (full(at.yn), full(at.yn), at.sib, full(at.ys)),
            (half(at.dg, 0), half(at.dg, 0), at.sib, half(at.ds, 0)),
            (half(at.dg, 1), half(at.dg, 1), at.sib, half(at.ds, 1)),
        )
        return route[k]

    def start(k, i):
        src, dst, dev, _ = hop(k, i)
        remote(src, dst, send_sems.at[k, i], recv_sems.at[k, i], dev).start()

    def arrived(k, i):
        src, _, dev, land = hop(k, i)
        remote(src, land, send_sems.at[k, i], recv_sems.at[k, i], dev).wait_recv()

    def sent(k, i):
        src, dst, dev, _ = hop(k, i)
        remote(src, dst, send_sems.at[k, i], recv_sems.at[k, i], dev).wait_send()

    def relay(i):
        arrived(0, i)
        start(3, i)
        start(5, i)
        arrived(1, i)
        start(4, i)
        start(6, i)

    def relay_diagonal(i):
        arrived(3, i)
        start(7, i)
        arrived(4, i)
        start(8, i)

    own = []
    for i, (_, buf, full, _) in enumerate(jobs):
        for copy in loads[i]:
            copy.wait()
        for k in range(3):
            start(k, i)
        own.append(pltpu.make_async_copy(buf, full(me), own_sems.at[i]))
        own[-1].start()
        if i == 0:
            share_gains()
            for copy in row_in[:2] + pack_in:
                copy.start()
        if i == 1:
            for copy in pack_in:
                copy.wait()
            for copy in pack_out:
                copy.start()
            normalize()
        if i >= 1:
            relay(i - 1)
        if i >= 2:
            relay_diagonal(i - 2)
    relay(count - 1)
    relay_diagonal(count - 2)
    relay_diagonal(count - 1)
    for i in range(count):
        for k in (2, 5, 6, 7, 8):
            arrived(k, i)
        for k in range(9):
            sent(k, i)
        own[i].wait()
    for copy in pack_out + row_out[-2:]:
        copy.wait()


def first_gather(gains, hidden, w_query, w_key, w_value, w_out, w_gate, w_up, w_down, n):
    hd, kd = w_query.shape[1:]
    d = w_out.shape[2]
    block = w_down.shape[1]
    rest = block - kd

    def plan(ins, outs, stage, keep):
        wq, wk, wv, wo, wg, wu, wd = ins
        gqkv, go, gg, gu, gd, pg, pd, pk, pv = outs
        cols, rows = stage
        kg, kdn, kk, kv = keep

        def by_columns(src, buf, first):
            column = lambda dev: pl.ds(pl.multiple_of(dev * kd, kd), kd)
            full = lambda dev: gqkv.at[pl.ds(first, hd), column(dev)]
            half = lambda dev, h: gqkv.at[pl.ds(first + h * (hd // 2), hd // 2), column(dev)]
            return [(src, buf)], buf, full, half

        def by_rows(pieces, buf, out):
            full = lambda dev: out.at[pl.ds(pl.multiple_of(dev * kd, kd), kd)]
            half = lambda dev, h: out.at[pl.ds(pl.multiple_of(dev * kd + h * (kd // 2), kd // 2), kd // 2)]
            return pieces, buf, full, half

        def blocks(w, first, size, buf):
            return [(w.at[0, :, pl.ds(e * block + first, size)], buf.at[:, pl.ds(e * size, size)]) for e in range(n)]

        jobs = [by_columns(w.at[0], cols.at[i], i * hd) for i, w in enumerate((wq, wk, wv))]
        jobs += [
            by_rows([(wo.at[0], rows.at[0])], rows.at[0], go),
            by_rows(blocks(wg, 0, kd, rows.at[1]), rows.at[1], gg), by_rows(blocks(wu, 0, kd, rows.at[2]), rows.at[2], gu),
            by_rows([(wd.at[0, pl.ds(0, kd)], rows.at[3])], rows.at[3], gd),
        ]
        pack_in = blocks(wg, kd, rest, kg.at[0]) + blocks(wu, kd, rest, kg.at[1])
        pack_in += [(wd.at[0, pl.ds(kd, rest)], kdn), (wk.at[1], kk), (wv.at[1], kv)]
        return jobs, pack_in, [(kg, pg), (kdn, pd), (kk, pk), (kv, pv)]

    count = 7
    shape = lambda *dims: jax.ShapeDtypeStruct(dims, BF16)
    outs = [jax.ShapeDtypeStruct((n,) + gains.shape, F32), shape(*hidden.shape)]
    outs += [shape(3 * hd, d)] + [shape(n * kd, d)] * 4
    outs += [shape(2, kd, n * rest), shape(rest, d), shape(hd, kd), shape(hd, kd)]
    batch, seq, _ = hidden.shape
    dma = pltpu.SemaphoreType.DMA
    return pl.pallas_call(
        functools.partial(gather_body, n, plan, 9, len(outs)),
        out_shape=outs,
        in_specs=[VM] + [HBM] * 8,
        out_specs=[VM] + [HBM] * (len(outs) - 1),
        scratch_shapes=[
            (pltpu.VMEM((3, hd, kd), BF16), pltpu.VMEM((4, kd, d), BF16)),
            (pltpu.VMEM((2, kd, n * rest), BF16), pltpu.VMEM((rest, d), BF16), pltpu.VMEM((hd, kd), BF16), pltpu.VMEM((hd, kd), BF16)),
            pltpu.VMEM((n,) + gains.shape, F32), pltpu.VMEM((1, d), F32),
            pltpu.VMEM((2, seq, d), BF16), pltpu.VMEM((2, seq, d), BF16),
            dma((5 + 2 * n,)), dma((2 * n + 3,)), dma((4,)), dma((n - 1,)), dma((n,)), dma((2, batch)),
            dma((count,)), dma((9, count)), dma((9, count)),
        ],
        compiler_params=params(48, 2),
        cost_estimate=cost(50_000_000_000, 50_000_000),
        name="first_gather",
    )(gains, hidden, w_query, w_key, w_value, w_out, w_gate, w_up, w_down)


GROUPS = 6
TABLE_STEP = 512


def tail_body(n, layer, o_ref, x_ref, gm_ref, gf_ref, wo_hbm, wg_hbm, wu_hbm, wd_hbm, emb_hbm, out_ref,
              wo, wg, wu, wd, emb, got, lhs, send, back, mid_ref, rows_ref, sib_send, sib_got, gate_send, gate_got, z_row, z_got, z_lhs,
              log_send, log_got, local_sems, pair_sems, send_sems, recv_sems):
    ex = Exchange(n, send_sems, recv_sems)
    me = ex.me
    pairs = ((wo_hbm.at[layer], wo), (wg_hbm.at[layer], wg), (wu_hbm.at[layer], wu), (wd_hbm.at[layer], wd), (emb_hbm, emb))
    loads = [pltpu.make_async_copy(src, dst, local_sems.at[i]) for i, (src, dst) in enumerate(pairs)]
    for load in loads:
        load.start()
    ex.barrier()

    x = spread(ex, 0, o_ref, got, lhs)
    loads[0].wait()
    mid = (x_ref[...] + reduce_rows(ex, 1, dot(x, wo[...]), send, back)).astype(BF16).astype(F32)
    mid_ref[...] = mid

    rows_ref[...] = rms_norm(mid, gm_ref[...]).astype(F32)
    x = spread(ex, 2, rows_ref, got, lhs)
    loads[1].wait()
    loads[2].wait()
    block = wd.shape[0]

    def gate_up(p):
        cols = pl.ds(pl.multiple_of(p * block, block), block)
        return dot(x, wg[:, cols]), dot(x, wu[:, cols])

    at = Place()
    across = (at.xs, at.ys, at.ds, at.sib)
    along = (at.xn, at.yn, at.dg, me)
    to_sib = [remote(sib_send.at[k], sib_got.at[k], pair_sems.at[0, k], pair_sems.at[1, k], at.sib) for k in range(4)]
    to_chip = [remote(gate_send.at[k], gate_got.at[k], pair_sems.at[2, k], pair_sems.at[3, k], along[k]) for k in range(3)]
    order = (2, 0, 1, 3)
    for k in order:
        gate, up = gate_up(across[k])
        sib_send[k, 0] = gate
        sib_send[k, 1] = up
        to_sib[k].start()
    for k in order:
        gate, up = gate_up(along[k])
        to_sib[k].wait_recv()
        gate = gate + sib_got[k, 0]
        up = up + sib_got[k, 1]
        if along[k] is not me:
            gate_send[k, 0] = gate
            gate_send[k, 1] = up
            to_chip[k].start()
    for k in range(3):
        to_chip[k].wait_recv()
        gate = gate + gate_got[k, 0]
        up = up + gate_got[k, 1]
    for copy in to_sib + to_chip:
        copy.wait_send()
    act = (gate * (1.0 / (1.0 + jnp.exp(-gate))) * up).astype(BF16)

    loads[3].wait()
    h = (mid_ref[...] + reduce_rows(ex, 4, dot(act, wd[...]), send, back)).astype(BF16).astype(F32)

    z_row[...] = rms_norm(h, gf_ref[...])
    rows = rows_ref.shape[0]
    ex.start(5, lambda j: z_row, z_got.at[me])
    z_got[me] = z_row[...]
    ex.wait(5, lambda j: z_row, lambda p: z_got.at[p])
    for i in range(n):
        z_lhs[pl.ds(i * rows, rows)] = z_got[i].astype(F32)
    z = z_lhs[...].astype(BF16)
    loads[4].wait()
    vocab = emb.shape[0]
    group = vocab // GROUPS
    for g in range(GROUPS):
        def step(c, carry):
            first = pl.multiple_of(g * group + c * TABLE_STEP, TABLE_STEP)
            part = dot_nt(z, emb[pl.ds(first, TABLE_STEP)])
            for i in range(n):
                log_send[i, :, pl.ds(first, TABLE_STEP)] = part[i * rows:(i + 1) * rows]
            return carry

        lax.fori_loop(0, group // TABLE_STEP, step, 0)
        src = lambda j, g=g: log_send.at[ex.peer(j), :, pl.ds(g * group, group)]
        dst = lambda p, g=g: log_got.at[:, pl.ds(pl.multiple_of(p * vocab + g * group, group), group)]
        ex.start(6 + g, src, dst(me))
    log_got[:, pl.ds(pl.multiple_of(me * vocab, vocab), vocab)] = log_send[me]
    for g in range(GROUPS):
        src = lambda j, g=g: log_send.at[ex.peer(j), :, pl.ds(g * group, group)]
        dst = lambda p, g=g: log_got.at[:, pl.ds(pl.multiple_of(p * vocab + g * group, group), group)]
        ex.wait(6 + g, src, dst)
    out_ref[...] = log_got[...]


def tail(o, x, gm, gf, w_out, w_gate, w_up, w_down, emb, layer, n):
    rows, d = x.shape
    kd, ffn, block, vocab = w_gate.shape[1], w_gate.shape[2], w_down.shape[1], emb.shape[0]
    stages = 6 + GROUPS
    weights = kd * d + 2 * kd * ffn + block * d + vocab * d
    return pl.pallas_call(
        functools.partial(tail_body, n, layer),
        out_shape=jax.ShapeDtypeStruct((rows, n * vocab), F32),
        in_specs=[VM, VM, VM, VM] + [HBM] * 5,
        out_specs=VM,
        scratch_shapes=[
            pltpu.VMEM((kd, d), BF16), pltpu.VMEM((kd, ffn), BF16), pltpu.VMEM((kd, ffn), BF16),
            pltpu.VMEM((block, d), BF16), pltpu.VMEM((vocab, d), BF16),
            pltpu.VMEM((n, rows, kd), F32), pltpu.VMEM((n * rows, kd), F32),
            pltpu.VMEM((n, rows, d), F32), pltpu.VMEM((n, rows, d), F32),
            pltpu.VMEM((rows, d), F32), pltpu.VMEM((rows, d), F32),
            pltpu.VMEM((4, 2, n * rows, block), F32), pltpu.VMEM((4, 2, n * rows, block), F32),
            pltpu.VMEM((3, 2, n * rows, block), F32), pltpu.VMEM((3, 2, n * rows, block), F32),
            pltpu.VMEM((rows, d), BF16), pltpu.VMEM((n, rows, d), BF16), pltpu.VMEM((n * rows, d), F32),
            pltpu.VMEM((n, rows, vocab), F32), pltpu.VMEM((rows, n * vocab), F32),
            pltpu.SemaphoreType.DMA((5,)), pltpu.SemaphoreType.DMA((4, 4)), pltpu.SemaphoreType.DMA((stages, n)), pltpu.SemaphoreType.DMA((stages, n)),
        ],
        compiler_params=params(58, 1),
        cost_estimate=cost(n * rows * weights, weights),
        name="tail",
    )(o, x, gm, gf, w_out, w_gate, w_up, w_down, emb)


def solution(mesh):
    row_spec = P(("part", "dp"))
    layer_spec = P(None, "dp")

    def device_step(hidden, prompt_lens, g_attn, w_query, w_key, w_value, w_out, g_mlp, w_gate, w_up, w_down, g_final, embedding):
        batch, seq_len, dim = hidden.shape
        heads, head_dim = w_query.shape[2], w_query.shape[3]
        n_dev = dim // w_query.shape[1]
        freqs = rope_frequencies(head_dim)
        angles = freqs[:, None] * np.arange(seq_len, dtype=np.float32)[None]
        cos_es, sin_es = jnp.asarray(np.cos(angles)), jnp.asarray(np.sin(angles))

        def headed(w):
            return w.transpose(0, 2, 3, 1).reshape(w.shape[0], heads * head_dim, -1)

        wq_t, wk_t, wv_t = headed(w_query), headed(w_key), headed(w_value)
        kd = dim // n_dev
        gains_loc = jnp.concatenate([g_attn, g_mlp, g_final[None], jnp.zeros((3, kd), BF16)], axis=0).astype(F32)
        gains, normed, gqkv, go, gg1, gup1, gd1, pg2, pd2, pk1, pv1 = first_gather(
            gains_loc, hidden, wq_t, wk_t, wv_t, w_out, w_gate, w_up, w_down, n_dev)
        gains = gains.transpose(1, 0, 2).reshape(8, dim)
        gu2 = lax.all_gather(pg2, "dp", axis=1, tiled=True)
        gd2 = lax.all_gather(pd2, "dp", axis=0, tiled=True)
        gk1 = lax.all_gather(pk1, "dp", axis=1, tiled=True)
        gv1 = lax.all_gather(pv1, "dp", axis=1, tiled=True)
        ga0, ga1, gm0, gm1, gf, *_ = gains
        hd = heads * head_dim

        lens = prompt_lens
        rope = (cos_es, sin_es, head_dim)
        rows = batch * seq_len
        q0, k_cache, v_cache = project(normed.reshape(rows, dim), gqkv, *rope, (True, True, False), (1, 2, 2), 0)
        attended = attention(lens, q0, k_cache, v_cache, head_dim)
        proj = jnp.einsum("bks,kd->bsd", attended, go, preferred_element_type=F32)
        mid = (hidden.astype(F32) + proj).astype(BF16)
        mid = mid.reshape(rows, dim)
        act, normed_mlp = gate_up(mid, gm0[None], (gg1, gup1), gg1.shape[1])
        part = down(act, gd1, rows)
        [act] = gate_up(normed_mlp, None, (gu2,), gu2.shape[2])
        h1 = down(act, gd2, BAND, (mid, part))

        last = lens - 1
        x = jnp.take_along_axis(h1.reshape(batch, seq_len, dim), last[:, None, None], axis=1, mode="clip")[:, 0]
        q1 = last_query(rms_norm(x, ga1).astype(F32), wq_t, 1, n_dev).reshape(batch, heads, head_dim)
        half = head_dim // 2
        turn = last.astype(F32)[:, None, None] * freqs
        cos_b, sin_b = jnp.cos(turn), jnp.sin(turn)
        low, high = q1[..., :half], q1[..., half:]
        q1 = jnp.concatenate([low * cos_b - high * sin_b, high * cos_b + low * sin_b], axis=-1).astype(BF16)
        own = np.arange(hd)[None, :] // head_dim == np.arange(heads)[:, None]
        q_diag = jnp.where(own[None], q1.reshape(batch, 1, hd), jnp.zeros((), BF16))

        k_cache, normed1 = project(h1, gk1, *rope, (True,), (2,), 1, k_cache, ga1[None])
        [v_cache] = project(normed1, gv1, *rope, (False,), (2,), 1, v_cache)

        o1 = last_attention(lens, q_diag, k_cache, v_cache, head_dim, 1)
        logits = tail(o1, x.astype(F32), gm1[None], gf[None], w_out, w_gate, w_up, w_down, embedding, 1, n_dev)

        def cache(c):
            return c.reshape(2, batch, heads, head_dim, seq_len).transpose(0, 1, 4, 2, 3)

        return cache(k_cache), cache(v_cache), logits

    cache_spec = P(None, ("part", "dp"))
    return jax.shard_map(
        device_step,
        mesh=mesh,
        in_specs=(row_spec, row_spec) + (layer_spec,) * 9 + (P("dp"), P("dp")),
        out_specs=(cache_spec, cache_spec, row_spec),
        check_vma=False,
    )
```

```python
import functools
import math
import jax
import jax.numpy as jnp
import numpy as np
from jax import lax
from jax.experimental import pallas as pl
from jax.experimental.pallas import tpu as pltpu
from jax.sharding import PartitionSpec as P

F32 = jnp.float32
BF16 = jnp.bfloat16
ANY = pl.BlockSpec(memory_space=pl.ANY)
HBM = pl.BlockSpec(memory_space=pltpu.HBM)
VM = pl.BlockSpec(memory_space=pltpu.VMEM)
NT = (((1,), (1,)), ((), ()))


def params(mib, collective=None):
    extra = {} if collective is None else dict(collective_id=collective, has_side_effects=True)
    return pltpu.CompilerParams(vmem_limit_bytes=mib << 20, **extra)


def cost(macs, values, exps=0):
    return pl.CostEstimate(flops=2 * macs, bytes_accessed=2 * values, transcendentals=exps)


def dot(a, b):
    return jnp.dot(a, b, preferred_element_type=F32)


def dot_nt(a, b):
    return lax.dot_general(a, b, NT, preferred_element_type=F32)


def rope_frequencies(head_dim):
    half_dim = head_dim // 2
    exponent = np.arange(half_dim, dtype=np.float32) * np.float32(2.0 / head_dim)
    inv_freq = np.float32(1.0) / np.float32(500000.0) ** exponent
    wave_len = np.float32(2.0 * math.pi) / inv_freq
    smooth = (np.float32(8192.0) / wave_len - np.float32(1.0)) / np.float32(3.0)
    blended = (1 - smooth) * inv_freq / 8 + smooth * inv_freq
    scaled = np.where(wave_len > 8192.0, inv_freq / 8, np.where(wave_len < 2048.0, inv_freq, blended))
    return scaled.astype(np.float32)


def rms_norm(values, gain_f32):
    values_f32 = values.astype(F32)
    mean_sq = jnp.mean(values_f32 * values_f32, axis=-1, keepdims=True)
    return (values_f32 * lax.rsqrt(mean_sq + 1e-5) * gain_f32).astype(BF16)


ROWS = 1024
PAIR = 2


def proj_body(ropes, per, head_dim, n_prev, norm, w_ref, a_ref, cos_ref, sin_ref, *rest):
    s = cos_ref.shape[1]
    half = head_dim // 2
    if norm:
        gain_ref, a_src, a_ref = rest[0], a_ref, rest[-1]
        rest = rest[1:-1]

        pl.when(pl.program_id(1) == 0)(lambda: normalize(a_src, gain_ref, a_ref))

    outs = rest[n_prev:]
    y = dot_nt(w_ref[...], a_ref[...])

    def store(rope, out_ref):
        for t in range(PAIR):
            part = y[:, t * s:(t + 1) * s]
            if not rope:
                out_ref[0, t] = part.astype(BF16)
                continue
            cos, sin = cos_ref[...], sin_ref[...]
            for i in range(ROWS // head_dim):
                low = part[i * head_dim:i * head_dim + half]
                high = part[i * head_dim + half:(i + 1) * head_dim]
                out_ref[0, t, pl.ds(i * head_dim, half)] = (low * cos - high * sin).astype(BF16)
                out_ref[0, t, pl.ds(i * head_dim + half, half)] = (high * cos + low * sin).astype(BF16)

    for k, (rope, out_ref) in enumerate(zip(ropes, outs)):
        pl.when(pl.program_id(1) // per == k)(functools.partial(store, rope, out_ref))


def project(a, w, cos, sin, head_dim, ropes, layers, layer, prev=None, gain=None):
    rows, d = a.shape
    s = cos.shape[1]
    b, width = rows // s, w.shape[0] // len(ropes)
    per = width // ROWS
    band = pl.BlockSpec((PAIR * s, d), lambda j, i: (j, 0))

    def place(k):
        def index(j, i):
            at = i - k * per
            waits = (at < 0) & (j > 0)
            return layer, jnp.where(waits, j - 1, j), jnp.where(waits, per - 1, jnp.clip(at, 0, per - 1)), 0
        return pl.BlockSpec((1, PAIR, ROWS, s), index)

    in_specs = [
        pl.BlockSpec((ROWS, d), lambda j, i: (i, 0)),
        band,
        pl.BlockSpec(cos.shape, lambda j, i: (0, 0)),
        pl.BlockSpec(sin.shape, lambda j, i: (0, 0)),
    ]
    args = [w, a, cos, sin]
    alias = {}
    out_shape = [jax.ShapeDtypeStruct((count, b, width, s), BF16) for count in layers]
    out_specs = [place(k) for k in range(len(ropes))]
    if gain is not None:
        in_specs.append(pl.BlockSpec(gain.shape, lambda i, j: (0, 0)))
        args.append(gain)
        out_shape.append(jax.ShapeDtypeStruct(a.shape, BF16))
        out_specs.append(band)
    if prev is not None:
        alias = {len(args): 0}
        in_specs.append(HBM)
        args.append(prev)
    return pl.pallas_call(
        functools.partial(proj_body, ropes, per, head_dim, len(alias), gain is not None),
        out_shape=out_shape,
        grid=(b // PAIR, w.shape[0] // ROWS),
        in_specs=in_specs,
        out_specs=out_specs,
        input_output_aliases=alias,
        compiler_params=params(58),
        cost_estimate=cost(rows * d * w.shape[0], w.size + a.size + a.size),
        name="project",
    )(*args)


TILE = 512
BAND = 1024


def normalize(src_ref, gain_ref, dst_ref):
    lines = 32

    def step(r, carry):
        rows = pl.ds(pl.multiple_of(r * lines, lines), lines)
        dst_ref[rows] = rms_norm(src_ref[rows], gain_ref[...])
        return carry

    lax.fori_loop(0, src_ref.shape[0] // lines, step, 0, unroll=4)


def gate_up_tile(x, wg_ref, wu_ref, o_ref):
    gate = dot(x, wg_ref[...])
    up = dot(x, wu_ref[...])
    o_ref[...] = (gate * (1.0 / (1.0 + jnp.exp(-gate))) * up).astype(BF16)


def gate_up_first_body(h_ref, gain_ref, wg_ref, wu_ref, o_ref, m_ref):
    @pl.when((pl.program_id(0) == 0) & (pl.program_id(1) == 0))
    def _():
        normalize(h_ref, gain_ref, m_ref)

    gate_up_tile(m_ref[pl.ds(pl.multiple_of(pl.program_id(1) * BAND, BAND), BAND)], wg_ref, wu_ref, o_ref)


def gate_up_rest_body(m_ref, wg_ref, wu_ref, o_ref):
    gate_up_tile(m_ref[pl.ds(pl.multiple_of(pl.program_id(1) * BAND, BAND), BAND)], wg_ref, wu_ref, o_ref)


def gate_up(rows_in, gain, weights, width):
    rows, d = rows_in.shape
    whole = pl.BlockSpec((rows, d), lambda i, j: (0, 0))
    out_shape = [jax.ShapeDtypeStruct((rows, width), BF16)]
    out_specs = [pl.BlockSpec((BAND, TILE), lambda i, j: (j, i))]
    if gain is not None:
        body, lead, args = gate_up_first_body, [whole, pl.BlockSpec(gain.shape, lambda i, j: (0, 0))], (rows_in, gain) + weights
        specs = [pl.BlockSpec((d, TILE), lambda i, j: (0, i))] * 2
        out_shape.append(jax.ShapeDtypeStruct((rows, d), BF16))
        out_specs.append(whole)
    else:
        body, lead, args = gate_up_rest_body, [whole], (rows_in,) + weights * 2
        specs = [pl.BlockSpec((None, d, TILE), lambda i, j, k=k: (k, 0, i)) for k in range(2)]
    return pl.pallas_call(
        body,
        out_shape=out_shape,
        grid=(width // TILE, rows // BAND),
        in_specs=lead + specs,
        out_specs=out_specs,
        compiler_params=params(60),
        cost_estimate=cost(2 * rows * d * width, 2 * d * width + rows * (d + width), rows * width),
        name="gate_up",
    )(*args)


def down_body(has_base, a_ref, w_ref, *rest):
    y = dot(a_ref[...], w_ref[...])
    if has_base:
        base_ref, part_ref, o_ref = rest
        o_ref[...] = (base_ref[...].astype(F32) + (part_ref[...] + y)).astype(BF16)
    else:
        rest[0][...] = y


def down(act, w, band, base=None):
    rows, kd = act.shape
    d = w.shape[1]
    tile = pl.BlockSpec((band, TILE), lambda i, j: (i, j))
    base = base or ()
    return pl.pallas_call(
        functools.partial(down_body, bool(base)),
        out_shape=jax.ShapeDtypeStruct((rows, d), BF16 if base else F32),
        grid=(rows // band, d // TILE),
        in_specs=[pl.BlockSpec((band, kd), lambda i, j: (i, 0)), pl.BlockSpec((kd, TILE), lambda i, j: (0, j))] + [tile] * len(base),
        out_specs=tile,
        compiler_params=params(60),
        cost_estimate=cost(rows * d * kd, rows * kd + kd * d + 3 * rows * d),
        name="down",
    )(act, w, *base)


HEADS_STEP = 8


def attn_body(head_dim, lens_ref, q_ref, k_ref, v_ref, o_ref):
    s = q_ref.shape[-1]
    length = lens_ref[pl.program_id(0)]
    t_pos = lax.broadcasted_iota(jnp.int32, (s, s), 0)
    s_pos = lax.broadcasted_iota(jnp.int32, (s, s), 1)
    allowed = (t_pos <= s_pos) & (t_pos < length)
    for i in range(HEADS_STEP):
        rows = pl.ds(i * head_dim, head_dim)
        q = q_ref[0, 0, rows] * jnp.asarray(head_dim ** -0.5, BF16)
        sc = lax.dot_general(k_ref[0, 0, rows], q, (((0,), (0,)), ((), ())), preferred_element_type=F32)
        sc = jnp.where(allowed, sc, -jnp.inf)
        ex = jnp.exp(sc - jnp.max(sc, axis=0, keepdims=True))
        p = (ex * (1.0 / jnp.sum(ex, axis=0, keepdims=True))).astype(BF16)
        o_ref[0, rows] = dot(v_ref[0, 0, rows], p).astype(BF16)


def attention(lens, q, k, v, head_dim):
    _, b, width, s = q.shape
    step = HEADS_STEP * head_dim
    spec = pl.BlockSpec((1, 1, step, s), lambda i, j, lens: (0, i, j, 0))
    return pl.pallas_call(
        functools.partial(attn_body, head_dim),
        out_shape=jax.ShapeDtypeStruct((b, width, s), BF16),
        grid_spec=pltpu.PrefetchScalarGridSpec(
            num_scalar_prefetch=1,
            grid=(b, width // step),
            in_specs=[spec, spec, spec],
            out_specs=pl.BlockSpec((1, step, s), lambda i, j, lens: (i, j, 0)),
        ),
        compiler_params=params(40),
        cost_estimate=cost(16 * b * s * s * width, 4 * b * s * width, b * s * s * width // head_dim),
        name="attention",
    )(lens, q, k, v)


def last_body(head_dim, lens_ref, q_ref, k_ref, v_ref, o_ref):
    length = lens_ref[pl.program_id(0)]
    sc = dot(q_ref[0], k_ref[0, 0]) * head_dim ** -0.5
    t_pos = lax.broadcasted_iota(jnp.int32, sc.shape, 1)
    sc = jnp.where(t_pos < length, sc, -jnp.inf)
    ex = jnp.exp(sc - jnp.max(sc, axis=-1, keepdims=True))
    p = (ex / jnp.sum(ex, axis=-1, keepdims=True)).astype(BF16)
    full = dot_nt(p, v_ref[0, 0])
    head = lax.broadcasted_iota(jnp.int32, full.shape, 0)
    col = lax.broadcasted_iota(jnp.int32, full.shape, 1)
    own = (col >= head * head_dim) & (col < (head + 1) * head_dim)
    o = jnp.sum(jnp.where(own, full, 0.0), axis=0, keepdims=True)
    o_ref[0] = o.astype(BF16).astype(F32)


def last_attention(lens, q_diag, k, v, head_dim, layer):
    b, heads, width = q_diag.shape
    s = k.shape[-1]
    kv = pl.BlockSpec((1, 1, width, s), lambda i, lens: (layer, i, 0, 0))
    return pl.pallas_call(
        functools.partial(last_body, head_dim),
        out_shape=jax.ShapeDtypeStruct((b, 1, width), F32),
        grid_spec=pltpu.PrefetchScalarGridSpec(
            num_scalar_prefetch=1,
            grid=(b,),
            in_specs=[pl.BlockSpec((1, heads, width), lambda i, lens: (i, 0, 0)), kv, kv],
            out_specs=pl.BlockSpec((1, 1, width), lambda i, lens: (i, 0, 0)),
        ),
        compiler_params=params(40),
        cost_estimate=cost(2 * b * s * width * heads, 2 * b * s * width, b * s * heads),
        name="last_attention",
    )(lens, q_diag, k, v)[:, 0]


class Exchange:
    def __init__(self, n, send_sems, recv_sems):
        self.n, self.send_sems, self.recv_sems = n, send_sems, recv_sems
        self.me = lax.axis_index("dp")

    def peer(self, j):
        return lax.rem(self.me + j, self.n)

    def barrier(self):
        sem = pltpu.get_barrier_semaphore()
        for j in range(1, self.n):
            pl.semaphore_signal(sem, inc=1, device_id={"dp": self.peer(j)}, device_id_type=pl.DeviceIdType.MESH)
        pl.semaphore_wait(sem, self.n - 1)

    def copy(self, stage, j, src, dst):
        return pltpu.make_async_remote_copy(
            src_ref=src, dst_ref=dst, send_sem=self.send_sems.at[stage, j], recv_sem=self.recv_sems.at[stage, self.me],
            device_id={"dp": self.peer(j)}, device_id_type=pl.DeviceIdType.MESH)

    def arrival(self, stage, j, src, dst):
        return pltpu.make_async_remote_copy(
            src_ref=src, dst_ref=dst, send_sem=self.send_sems.at[stage, j], recv_sem=self.recv_sems.at[stage, self.peer(j)],
            device_id={"dp": self.peer(j)}, device_id_type=pl.DeviceIdType.MESH)

    def start(self, stage, src_of, dst):
        for j in range(1, self.n):
            self.copy(stage, j, src_of(j), dst).start()

    def wait(self, stage, src_of, dst_from):
        for j in range(1, self.n):
            self.arrival(stage, j, src_of(j), dst_from(self.peer(j))).wait_recv()
        for j in range(1, self.n):
            self.arrival(stage, j, src_of(j), dst_from(self.peer(j))).wait_send()


def columns(ref, index, width):
    return ref.at[:, pl.ds(pl.multiple_of(index * width, width), width)]


def spread(ex, stage, rows_ref, got_ref, lhs_ref):
    n, rows, width = got_ref.shape
    src = lambda j: columns(rows_ref, ex.peer(j), width)
    ex.start(stage, src, got_ref.at[ex.me])
    got_ref[ex.me] = columns(rows_ref, ex.me, width)[...]
    ex.wait(stage, src, lambda p: got_ref.at[p])
    for i in range(n):
        lhs_ref[pl.ds(i * rows, rows)] = got_ref[i]
    return lhs_ref[...].astype(BF16)


def reduce_rows(ex, stage, part, send_ref, got_ref):
    n, rows, _ = got_ref.shape
    for i in range(n):
        send_ref[i] = part[i * rows:(i + 1) * rows]
    src = lambda j: send_ref.at[ex.peer(j)]
    ex.start(stage, src, got_ref.at[ex.me])
    got_ref[ex.me] = send_ref[ex.me]
    ex.wait(stage, src, lambda p: got_ref.at[p])
    total = got_ref[0]
    for i in range(1, n):
        total = total + got_ref[i]
    return total


def query_body(n, layer, a_ref, w_hbm, q_ref, w, got, lhs, send, back, local_sem, send_sems, recv_sems):
    load = pltpu.make_async_copy(w_hbm.at[layer], w, local_sem)
    load.start()
    ex = Exchange(n, send_sems, recv_sems)
    ex.barrier()
    x = spread(ex, 0, a_ref, got, lhs)
    load.wait()
    q_ref[...] = reduce_rows(ex, 1, dot_nt(x, w[...]), send, back)


def last_query(a_last, w_rows, layer, n):
    rows, d = a_last.shape
    _, width, kd = w_rows.shape
    return pl.pallas_call(
        functools.partial(query_body, n, layer),
        out_shape=jax.ShapeDtypeStruct((rows, width), F32),
        in_specs=[VM, HBM],
        out_specs=VM,
        scratch_shapes=[
            pltpu.VMEM((width, kd), BF16),
            pltpu.VMEM((n, rows, kd), F32), pltpu.VMEM((n * rows, kd), F32),
            pltpu.VMEM((n, rows, width), F32), pltpu.VMEM((n, rows, width), F32),
            pltpu.SemaphoreType.DMA, pltpu.SemaphoreType.DMA((2, n)), pltpu.SemaphoreType.DMA((2, n)),
        ],
        compiler_params=params(16, 0),
        cost_estimate=cost(n * rows * width * kd, width * kd),
        name="last_query",
    )(a_last, w_rows)


class Place:
    def __init__(self):
        me = lax.axis_index("dp")
        core, col, row = lax.rem(me, 2), lax.rem(me // 2, 2), me // 4
        at = lambda r, c, k: r * 4 + c * 2 + k
        self.me = me
        self.sib = at(row, col, 1 - core)
        self.xn, self.yn, self.dg = at(row, 1 - col, core), at(1 - row, col, core), at(1 - row, 1 - col, core)
        self.xs, self.ys, self.ds = at(row, 1 - col, 1 - core), at(1 - row, col, 1 - core), at(1 - row, 1 - col, 1 - core)


def remote(src, dst, send_sem, recv_sem, dev):
    return pltpu.make_async_remote_copy(src_ref=src, dst_ref=dst, send_sem=send_sem, recv_sem=recv_sem,
                                        device_id={"dp": dev}, device_id_type=pl.DeviceIdType.MESH)


def greet(devs):
    sem = pltpu.get_barrier_semaphore()
    for dev in devs:
        pl.semaphore_signal(sem, inc=1, device_id={"dp": dev}, device_id_type=pl.DeviceIdType.MESH)
    pl.semaphore_wait(sem, len(devs))


def gather_body(n, plan, n_in, n_out, *refs):
    ins, outs = refs[:n_in], refs[n_in:n_in + n_out]
    (stage, keep, gain_got, gain_row, raw, normed, load_sems, pack_sems, keep_sems, gain_send, gain_recv, row_sems, own_sems,
     send_sems, recv_sems) = refs[n_in + n_out:]
    at = Place()
    me = at.me
    gain_ref, hidden = ins[:2]
    gains_out, normed_out = outs[:2]
    jobs, pack_in, pack_out = plan(ins[2:], outs[2:], stage, keep)
    count = len(jobs)
    loads, taken = [], 0
    for pieces, _, _, _ in jobs:
        loads.append([pltpu.make_async_copy(src, dst, load_sems.at[taken + i]) for i, (src, dst) in enumerate(pieces)])
        taken += len(pieces)
    for copy in sum(loads, []):
        copy.start()
    batch = hidden.shape[0]
    row_in = [pltpu.make_async_copy(hidden.at[i], raw.at[i % 2], row_sems.at[0, i]) for i in range(batch)]
    row_out = [pltpu.make_async_copy(normed.at[i % 2], normed_out.at[i], row_sems.at[1, i]) for i in range(batch)]
    pack_in = [pltpu.make_async_copy(src, dst, pack_sems.at[i]) for i, (src, dst) in enumerate(pack_in)]
    pack_out = [pltpu.make_async_copy(src, dst, keep_sems.at[i]) for i, (src, dst) in enumerate(pack_out)]
    peers = [lax.rem(me + j, n) for j in range(1, n)]
    greet(peers)

    def gain_to(j):
        return remote(gain_ref, gain_got.at[me], gain_send.at[j], gain_recv.at[me], peers[j])

    def gain_from(j):
        return remote(gain_ref, gain_got.at[peers[j]], gain_send.at[j], gain_recv.at[peers[j]], peers[j])

    def share_gains():
        for j in range(n - 1):
            gain_to(j).start()
        gain_got[me] = gain_ref[...]

    def normalize():
        for j in range(n - 1):
            gain_from(j).wait_recv()
            gain_from(j).wait_send()
        gains_out[...] = gain_got[...]
        width = gain_ref.shape[1]
        for i in range(n):
            gain_row[:, pl.ds(i * width, width)] = gain_got[i, pl.ds(0, 1)]
        block = 32
        for i in range(batch):
            row_in[i].wait()
            if i >= 2:
                row_out[i - 2].wait()

            def step(r, carry, i=i):
                rows = pl.ds(pl.multiple_of(r * block, block), block)
                normed[i % 2, rows] = rms_norm(raw[i % 2, rows], gain_row[...])
                return carry

            lax.fori_loop(0, raw.shape[1] // block, step, 0)
            row_out[i].start()
            if i + 2 < batch:
                row_in[i + 2].start()

    def hop(k, i):
        _, buf, full, half = jobs[i]
        route = (
            (buf, full(at.me), at.xn, full(at.xn)),
            (buf, full(at.me), at.yn, full(at.yn)),
            (buf, full(at.me), at.sib, full(at.sib)),
            (half(at.xn, 0), half(at.xn, 0), at.yn, half(at.dg, 0)),
            (half(at.yn, 1), half(at.yn, 1), at.xn, half(at.dg, 1)),
            (full(at.xn), full(at.xn), at.sib, full(at.xs)),
            (full(at.yn), full(at.yn), at.sib, full(at.ys)),
            (half(at.dg, 0), half(at.dg, 0), at.sib, half(at.ds, 0)),
            (half(at.dg, 1), half(at.dg, 1), at.sib, half(at.ds, 1)),
        )
        return route[k]

    def start(k, i):
        src, dst, dev, _ = hop(k, i)
        remote(src, dst, send_sems.at[k, i], recv_sems.at[k, i], dev).start()

    def arrived(k, i):
        src, _, dev, land = hop(k, i)
        remote(src, land, send_sems.at[k, i], recv_sems.at[k, i], dev).wait_recv()

    def sent(k, i):
        src, dst, dev, _ = hop(k, i)
        remote(src, dst, send_sems.at[k, i], recv_sems.at[k, i], dev).wait_send()

    def relay(i):
        arrived(0, i)
        start(3, i)
        start(5, i)
        arrived(1, i)
        start(4, i)
        start(6, i)

    def relay_diagonal(i):
        arrived(3, i)
        start(7, i)
        arrived(4, i)
        start(8, i)

    own = []
    for i, (_, buf, full, _) in enumerate(jobs):
        for copy in loads[i]:
            copy.wait()
        for k in range(3):
            start(k, i)
        own.append(pltpu.make_async_copy(buf, full(me), own_sems.at[i]))
        own[-1].start()
        if i == 0:
            share_gains()
            for copy in row_in[:2] + pack_in:
                copy.start()
        if i == 1:
            for copy in pack_in:
                copy.wait()
            for copy in pack_out:
                copy.start()
            normalize()
        if i >= 1:
            relay(i - 1)
        if i >= 2:
            relay_diagonal(i - 2)
    relay(count - 1)
    relay_diagonal(count - 2)
    relay_diagonal(count - 1)
    for i in range(count):
        for k in (2, 5, 6, 7, 8):
            arrived(k, i)
        for k in range(9):
            sent(k, i)
        own[i].wait()
    for copy in pack_out + row_out[-2:]:
        copy.wait()


def first_gather(gains, hidden, w_query, w_key, w_value, w_out, w_gate, w_up, w_down, n):
    hd, kd = w_query.shape[1:]
    d = w_out.shape[2]
    block = w_down.shape[1]
    rest = block - kd

    def plan(ins, outs, stage, keep):
        wq, wk, wv, wo, wg, wu, wd = ins
        gqkv, go, gg, gu, gd, pg, pd, pk, pv = outs
        cols, rows = stage
        kg, kdn, kk, kv = keep

        def by_columns(src, buf, first):
            column = lambda dev: pl.ds(pl.multiple_of(dev * kd, kd), kd)
            full = lambda dev: gqkv.at[pl.ds(first, hd), column(dev)]
            half = lambda dev, h: gqkv.at[pl.ds(first + h * (hd // 2), hd // 2), column(dev)]
            return [(src, buf)], buf, full, half

        def by_rows(pieces, buf, out):
            full = lambda dev: out.at[pl.ds(pl.multiple_of(dev * kd, kd), kd)]
            half = lambda dev, h: out.at[pl.ds(pl.multiple_of(dev * kd + h * (kd // 2), kd // 2), kd // 2)]
            return pieces, buf, full, half

        def blocks(w, first, size, buf):
            return [(w.at[0, :, pl.ds(e * block + first, size)], buf.at[:, pl.ds(e * size, size)]) for e in range(n)]

        jobs = [by_columns(w.at[0], cols.at[i], i * hd) for i, w in enumerate((wq, wk, wv))]
        jobs += [
            by_rows([(wo.at[0], rows.at[0])], rows.at[0], go),
            by_rows(blocks(wg, 0, kd, rows.at[1]), rows.at[1], gg), by_rows(blocks(wu, 0, kd, rows.at[2]), rows.at[2], gu),
            by_rows([(wd.at[0, pl.ds(0, kd)], rows.at[3])], rows.at[3], gd),
        ]
        pack_in = blocks(wg, kd, rest, kg.at[0]) + blocks(wu, kd, rest, kg.at[1])
        pack_in += [(wd.at[0, pl.ds(kd, rest)], kdn), (wk.at[1], kk), (wv.at[1], kv)]
        return jobs, pack_in, [(kg, pg), (kdn, pd), (kk, pk), (kv, pv)]

    count = 7
    shape = lambda *dims: jax.ShapeDtypeStruct(dims, BF16)
    outs = [jax.ShapeDtypeStruct((n,) + gains.shape, F32), shape(*hidden.shape)]
    outs += [shape(3 * hd, d)] + [shape(n * kd, d)] * 4
    outs += [shape(2, kd, n * rest), shape(rest, d), shape(hd, kd), shape(hd, kd)]
    batch, seq, _ = hidden.shape
    dma = pltpu.SemaphoreType.DMA
    return pl.pallas_call(
        functools.partial(gather_body, n, plan, 9, len(outs)),
        out_shape=outs,
        in_specs=[VM] + [HBM] * 8,
        out_specs=[VM] + [HBM] * (len(outs) - 1),
        scratch_shapes=[
            (pltpu.VMEM((3, hd, kd), BF16), pltpu.VMEM((4, kd, d), BF16)),
            (pltpu.VMEM((2, kd, n * rest), BF16), pltpu.VMEM((rest, d), BF16), pltpu.VMEM((hd, kd), BF16), pltpu.VMEM((hd, kd), BF16)),
            pltpu.VMEM((n,) + gains.shape, F32), pltpu.VMEM((1, d), F32),
            pltpu.VMEM((2, seq, d), BF16), pltpu.VMEM((2, seq, d), BF16),
            dma((5 + 2 * n,)), dma((2 * n + 3,)), dma((4,)), dma((n - 1,)), dma((n,)), dma((2, batch)),
            dma((count,)), dma((9, count)), dma((9, count)),
        ],
        compiler_params=params(48, 2),
        cost_estimate=cost(50_000_000_000, 50_000_000),
        name="first_gather",
    )(gains, hidden, w_query, w_key, w_value, w_out, w_gate, w_up, w_down)


GROUPS = 6
TABLE_STEP = 512


def tail_body(n, layer, o_ref, x_ref, gm_ref, gf_ref, wo_hbm, wg_hbm, wu_hbm, wd_hbm, emb_hbm, out_ref,
              wo, wg, wu, wd, emb, got, lhs, send, back, mid_ref, rows_ref, sib_send, sib_got, gate_send, gate_got, z_row, z_got, z_lhs,
              log_send, log_got, local_sems, pair_sems, send_sems, recv_sems):
    ex = Exchange(n, send_sems, recv_sems)
    me = ex.me
    pairs = ((wo_hbm.at[layer], wo), (wg_hbm.at[layer], wg), (wu_hbm.at[layer], wu), (wd_hbm.at[layer], wd), (emb_hbm, emb))
    loads = [pltpu.make_async_copy(src, dst, local_sems.at[i]) for i, (src, dst) in enumerate(pairs)]
    for load in loads:
        load.start()
    ex.barrier()

    x = spread(ex, 0, o_ref, got, lhs)
    loads[0].wait()
    mid = (x_ref[...] + reduce_rows(ex, 1, dot(x, wo[...]), send, back)).astype(BF16).astype(F32)
    mid_ref[...] = mid

    rows_ref[...] = rms_norm(mid, gm_ref[...]).astype(F32)
    x = spread(ex, 2, rows_ref, got, lhs)
    loads[1].wait()
    loads[2].wait()
    block = wd.shape[0]

    def gate_up(p):
        cols = pl.ds(pl.multiple_of(p * block, block), block)
        return dot(x, wg[:, cols]), dot(x, wu[:, cols])

    at = Place()
    across = (at.xs, at.ys, at.ds, at.sib)
    along = (at.xn, at.yn, at.dg, me)
    to_sib = [remote(sib_send.at[k], sib_got.at[k], pair_sems.at[0, k], pair_sems.at[1, k], at.sib) for k in range(4)]
    to_chip = [remote(gate_send.at[k], gate_got.at[k], pair_sems.at[2, k], pair_sems.at[3, k], along[k]) for k in range(3)]

    def pass_across(k):
        sib_send[k, 0], sib_send[k, 1] = gate_up(across[k])
        to_sib[k].start()

    def pass_along(k):
        gate, up = gate_up(along[k])
        to_sib[k].wait_recv()
        gate = gate + sib_got[k, 0]
        up = up + sib_got[k, 1]
        if along[k] is not me:
            gate_send[k, 0], gate_send[k, 1] = gate, up
            to_chip[k].start()
        return gate, up

    order = (2, 0, 1, 3)
    pass_across(order[0])
    for k, after in zip(order, order[1:]):
        pass_across(after)
        pass_along(k)
    gate, up = pass_along(order[-1])
    for k in range(3):
        to_chip[k].wait_recv()
        gate = gate + gate_got[k, 0]
        up = up + gate_got[k, 1]
    for copy in to_sib + to_chip:
        copy.wait_send()
    act = (gate * (1.0 / (1.0 + jnp.exp(-gate))) * up).astype(BF16)

    loads[3].wait()
    h = (mid_ref[...] + reduce_rows(ex, 4, dot(act, wd[...]), send, back)).astype(BF16).astype(F32)

    z_row[...] = rms_norm(h, gf_ref[...])
    rows = rows_ref.shape[0]
    ex.start(5, lambda j: z_row, z_got.at[me])
    z_got[me] = z_row[...]
    ex.wait(5, lambda j: z_row, lambda p: z_got.at[p])
    for i in range(n):
        z_lhs[pl.ds(i * rows, rows)] = z_got[i].astype(F32)
    z = z_lhs[...].astype(BF16)
    loads[4].wait()
    vocab = emb.shape[0]
    group = vocab // GROUPS
    for g in range(GROUPS):
        def step(c, carry):
            first = pl.multiple_of(g * group + c * TABLE_STEP, TABLE_STEP)
            part = dot_nt(z, emb[pl.ds(first, TABLE_STEP)])
            for i in range(n):
                log_send[i, :, pl.ds(first, TABLE_STEP)] = part[i * rows:(i + 1) * rows]
            return carry

        lax.fori_loop(0, group // TABLE_STEP, step, 0)
        src = lambda j, g=g: log_send.at[ex.peer(j), :, pl.ds(g * group, group)]
        dst = lambda p, g=g: log_got.at[:, pl.ds(pl.multiple_of(p * vocab + g * group, group), group)]
        ex.start(6 + g, src, dst(me))
    log_got[:, pl.ds(pl.multiple_of(me * vocab, vocab), vocab)] = log_send[me]
    for g in range(GROUPS):
        src = lambda j, g=g: log_send.at[ex.peer(j), :, pl.ds(g * group, group)]
        dst = lambda p, g=g: log_got.at[:, pl.ds(pl.multiple_of(p * vocab + g * group, group), group)]
        ex.wait(6 + g, src, dst)
    out_ref[...] = log_got[...]


def tail(o, x, gm, gf, w_out, w_gate, w_up, w_down, emb, layer, n):
    rows, d = x.shape
    kd, ffn, block, vocab = w_gate.shape[1], w_gate.shape[2], w_down.shape[1], emb.shape[0]
    stages = 6 + GROUPS
    weights = kd * d + 2 * kd * ffn + block * d + vocab * d
    return pl.pallas_call(
        functools.partial(tail_body, n, layer),
        out_shape=jax.ShapeDtypeStruct((rows, n * vocab), F32),
        in_specs=[VM, VM, VM, VM] + [HBM] * 5,
        out_specs=VM,
        scratch_shapes=[
            pltpu.VMEM((kd, d), BF16), pltpu.VMEM((kd, ffn), BF16), pltpu.VMEM((kd, ffn), BF16),
            pltpu.VMEM((block, d), BF16), pltpu.VMEM((vocab, d), BF16),
            pltpu.VMEM((n, rows, kd), F32), pltpu.VMEM((n * rows, kd), F32),
            pltpu.VMEM((n, rows, d), F32), pltpu.VMEM((n, rows, d), F32),
            pltpu.VMEM((rows, d), F32), pltpu.VMEM((rows, d), F32),
            pltpu.VMEM((4, 2, n * rows, block), F32), pltpu.VMEM((4, 2, n * rows, block), F32),
            pltpu.VMEM((3, 2, n * rows, block), F32), pltpu.VMEM((3, 2, n * rows, block), F32),
            pltpu.VMEM((rows, d), BF16), pltpu.VMEM((n, rows, d), BF16), pltpu.VMEM((n * rows, d), F32),
            pltpu.VMEM((n, rows, vocab), F32), pltpu.VMEM((rows, n * vocab), F32),
            pltpu.SemaphoreType.DMA((5,)), pltpu.SemaphoreType.DMA((4, 4)), pltpu.SemaphoreType.DMA((stages, n)), pltpu.SemaphoreType.DMA((stages, n)),
        ],
        compiler_params=params(58, 1),
        cost_estimate=cost(n * rows * weights, weights),
        name="tail",
    )(o, x, gm, gf, w_out, w_gate, w_up, w_down, emb)


def solution(mesh):
    row_spec = P(("part", "dp"))
    layer_spec = P(None, "dp")

    def device_step(hidden, prompt_lens, g_attn, w_query, w_key, w_value, w_out, g_mlp, w_gate, w_up, w_down, g_final, embedding):
        batch, seq_len, dim = hidden.shape
        heads, head_dim = w_query.shape[2], w_query.shape[3]
        n_dev = dim // w_query.shape[1]
        freqs = rope_frequencies(head_dim)
        angles = freqs[:, None] * np.arange(seq_len, dtype=np.float32)[None]
        cos_es, sin_es = jnp.asarray(np.cos(angles)), jnp.asarray(np.sin(angles))

        def headed(w):
            return w.transpose(0, 2, 3, 1).reshape(w.shape[0], heads * head_dim, -1)

        wq_t, wk_t, wv_t = headed(w_query), headed(w_key), headed(w_value)
        kd = dim // n_dev
        gains_loc = jnp.concatenate([g_attn, g_mlp, g_final[None], jnp.zeros((3, kd), BF16)], axis=0).astype(F32)
        gains, normed, gqkv, go, gg1, gup1, gd1, pg2, pd2, pk1, pv1 = first_gather(
            gains_loc, hidden, wq_t, wk_t, wv_t, w_out, w_gate, w_up, w_down, n_dev)
        gains = gains.transpose(1, 0, 2).reshape(8, dim)
        gu2 = lax.all_gather(pg2, "dp", axis=1, tiled=True)
        gd2 = lax.all_gather(pd2, "dp", axis=0, tiled=True)
        gk1 = lax.all_gather(pk1, "dp", axis=1, tiled=True)
        gv1 = lax.all_gather(pv1, "dp", axis=1, tiled=True)
        ga0, ga1, gm0, gm1, gf, *_ = gains
        hd = heads * head_dim

        lens = prompt_lens
        rope = (cos_es, sin_es, head_dim)
        rows = batch * seq_len
        q0, k_cache, v_cache = project(normed.reshape(rows, dim), gqkv, *rope, (True, True, False), (1, 2, 2), 0)
        attended = attention(lens, q0, k_cache, v_cache, head_dim)
        proj = jnp.einsum("bks,kd->bsd", attended, go, preferred_element_type=F32)
        mid = (hidden.astype(F32) + proj).astype(BF16)
        mid = mid.reshape(rows, dim)
        act, normed_mlp = gate_up(mid, gm0[None], (gg1, gup1), gg1.shape[1])
        part = down(act, gd1, rows)
        [act] = gate_up(normed_mlp, None, (gu2,), gu2.shape[2])
        h1 = down(act, gd2, BAND, (mid, part))

        last = lens - 1
        x = jnp.take_along_axis(h1.reshape(batch, seq_len, dim), last[:, None, None], axis=1, mode="clip")[:, 0]
        q1 = last_query(rms_norm(x, ga1).astype(F32), wq_t, 1, n_dev).reshape(batch, heads, head_dim)
        half = head_dim // 2
        turn = last.astype(F32)[:, None, None] * freqs
        cos_b, sin_b = jnp.cos(turn), jnp.sin(turn)
        low, high = q1[..., :half], q1[..., half:]
        q1 = jnp.concatenate([low * cos_b - high * sin_b, high * cos_b + low * sin_b], axis=-1).astype(BF16)
        own = np.arange(hd)[None, :] // head_dim == np.arange(heads)[:, None]
        q_diag = jnp.where(own[None], q1.reshape(batch, 1, hd), jnp.zeros((), BF16))

        k_cache, normed1 = project(h1, gk1, *rope, (True,), (2,), 1, k_cache, ga1[None])
        [v_cache] = project(normed1, gv1, *rope, (False,), (2,), 1, v_cache)

        o1 = last_attention(lens, q_diag, k_cache, v_cache, head_dim, 1)
        logits = tail(o1, x.astype(F32), gm1[None], gf[None], w_out, w_gate, w_up, w_down, embedding, 1, n_dev)

        def cache(c):
            return c.reshape(2, batch, heads, head_dim, seq_len).transpose(0, 1, 4, 2, 3)

        return cache(k_cache), cache(v_cache), logits

    cache_spec = P(None, ("part", "dp"))
    return jax.shard_map(
        device_step,
        mesh=mesh,
        in_specs=(row_spec, row_spec) + (layer_spec,) * 9 + (P("dp"), P("dp")),
        out_specs=(cache_spec, cache_spec, row_spec),
        check_vma=False,
    )
```

```python
import functools
import math
import jax
import jax.numpy as jnp
import numpy as np
from jax import lax
from jax.experimental import pallas as pl
from jax.experimental.pallas import tpu as pltpu
from jax.sharding import PartitionSpec as P

F32 = jnp.float32
BF16 = jnp.bfloat16
ANY = pl.BlockSpec(memory_space=pl.ANY)
HBM = pl.BlockSpec(memory_space=pltpu.HBM)
VM = pl.BlockSpec(memory_space=pltpu.VMEM)
NT = (((1,), (1,)), ((), ()))


def params(mib, collective=None):
    extra = {} if collective is None else dict(collective_id=collective, has_side_effects=True)
    return pltpu.CompilerParams(vmem_limit_bytes=mib << 20, **extra)


def cost(macs, values, exps=0):
    return pl.CostEstimate(flops=2 * macs, bytes_accessed=2 * values, transcendentals=exps)


def dot(a, b):
    return jnp.dot(a, b, preferred_element_type=F32)


def dot_nt(a, b):
    return lax.dot_general(a, b, NT, preferred_element_type=F32)


def rope_frequencies(head_dim):
    half_dim = head_dim // 2
    exponent = np.arange(half_dim, dtype=np.float32) * np.float32(2.0 / head_dim)
    inv_freq = np.float32(1.0) / np.float32(500000.0) ** exponent
    wave_len = np.float32(2.0 * math.pi) / inv_freq
    smooth = (np.float32(8192.0) / wave_len - np.float32(1.0)) / np.float32(3.0)
    blended = (1 - smooth) * inv_freq / 8 + smooth * inv_freq
    scaled = np.where(wave_len > 8192.0, inv_freq / 8, np.where(wave_len < 2048.0, inv_freq, blended))
    return scaled.astype(np.float32)


def rms_norm(values, gain_f32):
    values_f32 = values.astype(F32)
    mean_sq = jnp.mean(values_f32 * values_f32, axis=-1, keepdims=True)
    return (values_f32 * lax.rsqrt(mean_sq + 1e-5) * gain_f32).astype(BF16)


ROWS = 1024
PAIR = 2


def proj_body(ropes, per, head_dim, n_prev, norm, w_ref, a_ref, cos_ref, sin_ref, *rest):
    s = cos_ref.shape[1]
    half = head_dim // 2
    if norm:
        gain_ref, a_src, a_ref = rest[0], a_ref, rest[-1]
        rest = rest[1:-1]

        pl.when(pl.program_id(1) == 0)(lambda: normalize(a_src, gain_ref, a_ref))

    outs = rest[n_prev:]
    y = dot_nt(w_ref[...], a_ref[...])

    def store(rope, out_ref):
        for t in range(PAIR):
            part = y[:, t * s:(t + 1) * s]
            if not rope:
                out_ref[0, t] = part.astype(BF16)
                continue
            cos, sin = cos_ref[...], sin_ref[...]
            for i in range(ROWS // head_dim):
                low = part[i * head_dim:i * head_dim + half]
                high = part[i * head_dim + half:(i + 1) * head_dim]
                out_ref[0, t, pl.ds(i * head_dim, half)] = (low * cos - high * sin).astype(BF16)
                out_ref[0, t, pl.ds(i * head_dim + half, half)] = (high * cos + low * sin).astype(BF16)

    for k, (rope, out_ref) in enumerate(zip(ropes, outs)):
        pl.when(pl.program_id(1) // per == k)(functools.partial(store, rope, out_ref))


def project(a, w, cos, sin, head_dim, ropes, layers, layer, prev=None, gain=None):
    rows, d = a.shape
    s = cos.shape[1]
    b, width = rows // s, w.shape[0] // len(ropes)
    per = width // ROWS
    band = pl.BlockSpec((PAIR * s, d), lambda j, i: (j, 0))

    def place(k):
        def index(j, i):
            at = i - k * per
            waits = (at < 0) & (j > 0)
            return layer, jnp.where(waits, j - 1, j), jnp.where(waits, per - 1, jnp.clip(at, 0, per - 1)), 0
        return pl.BlockSpec((1, PAIR, ROWS, s), index)

    in_specs = [
        pl.BlockSpec((ROWS, d), lambda j, i: (i, 0)),
        band,
        pl.BlockSpec(cos.shape, lambda j, i: (0, 0)),
        pl.BlockSpec(sin.shape, lambda j, i: (0, 0)),
    ]
    args = [w, a, cos, sin]
    alias = {}
    out_shape = [jax.ShapeDtypeStruct((count, b, width, s), BF16) for count in layers]
    out_specs = [place(k) for k in range(len(ropes))]
    if gain is not None:
        in_specs.append(pl.BlockSpec(gain.shape, lambda i, j: (0, 0)))
        args.append(gain)
        out_shape.append(jax.ShapeDtypeStruct(a.shape, BF16))
        out_specs.append(band)
    if prev is not None:
        alias = {len(args): 0}
        in_specs.append(HBM)
        args.append(prev)
    return pl.pallas_call(
        functools.partial(proj_body, ropes, per, head_dim, len(alias), gain is not None),
        out_shape=out_shape,
        grid=(b // PAIR, w.shape[0] // ROWS),
        in_specs=in_specs,
        out_specs=out_specs,
        input_output_aliases=alias,
        compiler_params=params(58),
        cost_estimate=cost(rows * d * w.shape[0], w.size + a.size + a.size),
        name="project",
    )(*args)


TILE = 512
BAND = 1024


def normalize(src_ref, gain_ref, dst_ref):
    lines = 32

    def step(r, carry):
        rows = pl.ds(pl.multiple_of(r * lines, lines), lines)
        dst_ref[rows] = rms_norm(src_ref[rows], gain_ref[...])
        return carry

    lax.fori_loop(0, src_ref.shape[0] // lines, step, 0, unroll=4)


def gate_up_tile(x, wg_ref, wu_ref, o_ref):
    gate = dot(x, wg_ref[...])
    up = dot(x, wu_ref[...])
    o_ref[...] = (gate * (1.0 / (1.0 + jnp.exp(-gate))) * up).astype(BF16)


def gate_up_first_body(h_ref, gain_ref, wg_ref, wu_ref, o_ref, m_ref):
    @pl.when((pl.program_id(0) == 0) & (pl.program_id(1) == 0))
    def _():
        normalize(h_ref, gain_ref, m_ref)

    gate_up_tile(m_ref[pl.ds(pl.multiple_of(pl.program_id(1) * BAND, BAND), BAND)], wg_ref, wu_ref, o_ref)


def gate_up_rest_body(m_ref, wg_ref, wu_ref, o_ref):
    gate_up_tile(m_ref[pl.ds(pl.multiple_of(pl.program_id(1) * BAND, BAND), BAND)], wg_ref, wu_ref, o_ref)


def gate_up(rows_in, gain, weights, width):
    rows, d = rows_in.shape
    whole = pl.BlockSpec((rows, d), lambda i, j: (0, 0))
    out_shape = [jax.ShapeDtypeStruct((rows, width), BF16)]
    out_specs = [pl.BlockSpec((BAND, TILE), lambda i, j: (j, i))]
    if gain is not None:
        body, lead, args = gate_up_first_body, [whole, pl.BlockSpec(gain.shape, lambda i, j: (0, 0))], (rows_in, gain) + weights
        specs = [pl.BlockSpec((d, TILE), lambda i, j: (0, i))] * 2
        out_shape.append(jax.ShapeDtypeStruct((rows, d), BF16))
        out_specs.append(whole)
    else:
        body, lead, args = gate_up_rest_body, [whole], (rows_in,) + weights * 2
        specs = [pl.BlockSpec((None, d, TILE), lambda i, j, k=k: (k, 0, i)) for k in range(2)]
    return pl.pallas_call(
        body,
        out_shape=out_shape,
        grid=(width // TILE, rows // BAND),
        in_specs=lead + specs,
        out_specs=out_specs,
        compiler_params=params(60),
        cost_estimate=cost(2 * rows * d * width, 2 * d * width + rows * (d + width), rows * width),
        name="gate_up",
    )(*args)


def down_body(has_base, a_ref, w_ref, *rest):
    y = dot(a_ref[...], w_ref[...])
    if has_base:
        base_ref, part_ref, o_ref = rest
        o_ref[...] = (base_ref[...].astype(F32) + (part_ref[...] + y)).astype(BF16)
    else:
        rest[0][...] = y


def down(act, w, band, base=None):
    rows, kd = act.shape
    d = w.shape[1]
    tile = pl.BlockSpec((band, TILE), lambda i, j: (i, j))
    base = base or ()
    return pl.pallas_call(
        functools.partial(down_body, bool(base)),
        out_shape=jax.ShapeDtypeStruct((rows, d), BF16 if base else F32),
        grid=(rows // band, d // TILE),
        in_specs=[pl.BlockSpec((band, kd), lambda i, j: (i, 0)), pl.BlockSpec((kd, TILE), lambda i, j: (0, j))] + [tile] * len(base),
        out_specs=tile,
        compiler_params=params(60),
        cost_estimate=cost(rows * d * kd, rows * kd + kd * d + 3 * rows * d),
        name="down",
    )(act, w, *base)


HEADS_STEP = 8


def attn_body(head_dim, lens_ref, q_ref, k_ref, v_ref, o_ref):
    s = q_ref.shape[-1]
    length = lens_ref[pl.program_id(0)]
    t_pos = lax.broadcasted_iota(jnp.int32, (s, s), 0)
    s_pos = lax.broadcasted_iota(jnp.int32, (s, s), 1)
    allowed = (t_pos <= s_pos) & (t_pos < length)
    for i in range(HEADS_STEP):
        rows = pl.ds(i * head_dim, head_dim)
        q = q_ref[0, 0, rows] * jnp.asarray(head_dim ** -0.5, BF16)
        sc = lax.dot_general(k_ref[0, 0, rows], q, (((0,), (0,)), ((), ())), preferred_element_type=F32)
        sc = jnp.where(allowed, sc, -jnp.inf)
        ex = jnp.exp(sc - jnp.max(sc, axis=0, keepdims=True))
        p = (ex * (1.0 / jnp.sum(ex, axis=0, keepdims=True))).astype(BF16)
        o_ref[0, rows] = dot(v_ref[0, 0, rows], p).astype(BF16)


def attention(lens, q, k, v, head_dim):
    _, b, width, s = q.shape
    step = HEADS_STEP * head_dim
    spec = pl.BlockSpec((1, 1, step, s), lambda i, j, lens: (0, i, j, 0))
    return pl.pallas_call(
        functools.partial(attn_body, head_dim),
        out_shape=jax.ShapeDtypeStruct((b, width, s), BF16),
        grid_spec=pltpu.PrefetchScalarGridSpec(
            num_scalar_prefetch=1,
            grid=(b, width // step),
            in_specs=[spec, spec, spec],
            out_specs=pl.BlockSpec((1, step, s), lambda i, j, lens: (i, j, 0)),
        ),
        compiler_params=params(40),
        cost_estimate=cost(16 * b * s * s * width, 4 * b * s * width, b * s * s * width // head_dim),
        name="attention",
    )(lens, q, k, v)


def last_body(head_dim, lens_ref, q_ref, k_ref, v_ref, o_ref):
    length = lens_ref[pl.program_id(0)]
    sc = dot(q_ref[0], k_ref[0, 0]) * head_dim ** -0.5
    t_pos = lax.broadcasted_iota(jnp.int32, sc.shape, 1)
    sc = jnp.where(t_pos < length, sc, -jnp.inf)
    ex = jnp.exp(sc - jnp.max(sc, axis=-1, keepdims=True))
    p = (ex / jnp.sum(ex, axis=-1, keepdims=True)).astype(BF16)
    full = dot_nt(p, v_ref[0, 0])
    head = lax.broadcasted_iota(jnp.int32, full.shape, 0)
    col = lax.broadcasted_iota(jnp.int32, full.shape, 1)
    own = (col >= head * head_dim) & (col < (head + 1) * head_dim)
    o = jnp.sum(jnp.where(own, full, 0.0), axis=0, keepdims=True)
    o_ref[0] = o.astype(BF16).astype(F32)


def last_attention(lens, q_diag, k, v, head_dim, layer):
    b, heads, width = q_diag.shape
    s = k.shape[-1]
    parts = 2
    kv = pl.BlockSpec((1, 1, width // parts, s), lambda i, p, lens: (layer, i, p, 0))
    return pl.pallas_call(
        functools.partial(last_body, head_dim),
        out_shape=jax.ShapeDtypeStruct((b, 1, width), F32),
        grid_spec=pltpu.PrefetchScalarGridSpec(
            num_scalar_prefetch=1,
            grid=(b, parts),
            in_specs=[pl.BlockSpec((1, heads // parts, width // parts), lambda i, p, lens: (i, p, p)), kv, kv],
            out_specs=pl.BlockSpec((1, 1, width // parts), lambda i, p, lens: (i, 0, p)),
        ),
        compiler_params=params(40),
        cost_estimate=cost(2 * b * s * width * heads, 2 * b * s * width, b * s * heads),
        name="last_attention",
    )(lens, q_diag, k, v)[:, 0]


class Exchange:
    def __init__(self, n, send_sems, recv_sems):
        self.n, self.send_sems, self.recv_sems = n, send_sems, recv_sems
        self.me = lax.axis_index("dp")

    def peer(self, j):
        return lax.rem(self.me + j, self.n)

    def barrier(self):
        sem = pltpu.get_barrier_semaphore()
        for j in range(1, self.n):
            pl.semaphore_signal(sem, inc=1, device_id={"dp": self.peer(j)}, device_id_type=pl.DeviceIdType.MESH)
        pl.semaphore_wait(sem, self.n - 1)

    def copy(self, stage, j, src, dst):
        return pltpu.make_async_remote_copy(
            src_ref=src, dst_ref=dst, send_sem=self.send_sems.at[stage, j], recv_sem=self.recv_sems.at[stage, self.me],
            device_id={"dp": self.peer(j)}, device_id_type=pl.DeviceIdType.MESH)

    def arrival(self, stage, j, src, dst):
        return pltpu.make_async_remote_copy(
            src_ref=src, dst_ref=dst, send_sem=self.send_sems.at[stage, j], recv_sem=self.recv_sems.at[stage, self.peer(j)],
            device_id={"dp": self.peer(j)}, device_id_type=pl.DeviceIdType.MESH)

    def start(self, stage, src_of, dst):
        for j in range(1, self.n):
            self.copy(stage, j, src_of(j), dst).start()

    def wait(self, stage, src_of, dst_from):
        for j in range(1, self.n):
            self.arrival(stage, j, src_of(j), dst_from(self.peer(j))).wait_recv()
        for j in range(1, self.n):
            self.arrival(stage, j, src_of(j), dst_from(self.peer(j))).wait_send()


def columns(ref, index, width):
    return ref.at[:, pl.ds(pl.multiple_of(index * width, width), width)]


def spread(ex, stage, rows_ref, got_ref, lhs_ref):
    n, rows, width = got_ref.shape
    src = lambda j: columns(rows_ref, ex.peer(j), width)
    ex.start(stage, src, got_ref.at[ex.me])
    got_ref[ex.me] = columns(rows_ref, ex.me, width)[...]
    ex.wait(stage, src, lambda p: got_ref.at[p])
    for i in range(n):
        lhs_ref[pl.ds(i * rows, rows)] = got_ref[i]
    return lhs_ref[...].astype(BF16)


def reduce_rows(ex, stage, part, send_ref, got_ref):
    n, rows, _ = got_ref.shape
    for i in range(n):
        send_ref[i] = part[i * rows:(i + 1) * rows]
    src = lambda j: send_ref.at[ex.peer(j)]
    ex.start(stage, src, got_ref.at[ex.me])
    got_ref[ex.me] = send_ref[ex.me]
    ex.wait(stage, src, lambda p: got_ref.at[p])
    total = got_ref[0]
    for i in range(1, n):
        total = total + got_ref[i]
    return total


def query_body(n, layer, a_ref, w_hbm, q_ref, w, got, lhs, send, back, local_sem, send_sems, recv_sems):
    load = pltpu.make_async_copy(w_hbm.at[layer], w, local_sem)
    load.start()
    ex = Exchange(n, send_sems, recv_sems)
    ex.barrier()
    x = spread(ex, 0, a_ref, got, lhs)
    load.wait()
    q_ref[...] = reduce_rows(ex, 1, dot_nt(x, w[...]), send, back)


def last_query(a_last, w_rows, layer, n):
    rows, d = a_last.shape
    _, width, kd = w_rows.shape
    return pl.pallas_call(
        functools.partial(query_body, n, layer),
        out_shape=jax.ShapeDtypeStruct((rows, width), F32),
        in_specs=[VM, HBM],
        out_specs=VM,
        scratch_shapes=[
            pltpu.VMEM((width, kd), BF16),
            pltpu.VMEM((n, rows, kd), F32), pltpu.VMEM((n * rows, kd), F32),
            pltpu.VMEM((n, rows, width), F32), pltpu.VMEM((n, rows, width), F32),
            pltpu.SemaphoreType.DMA, pltpu.SemaphoreType.DMA((2, n)), pltpu.SemaphoreType.DMA((2, n)),
        ],
        compiler_params=params(16, 0),
        cost_estimate=cost(n * rows * width * kd, width * kd),
        name="last_query",
    )(a_last, w_rows)


class Place:
    def __init__(self):
        me = lax.axis_index("dp")
        core, col, row = lax.rem(me, 2), lax.rem(me // 2, 2), me // 4
        at = lambda r, c, k: r * 4 + c * 2 + k
        self.me = me
        self.sib = at(row, col, 1 - core)
        self.xn, self.yn, self.dg = at(row, 1 - col, core), at(1 - row, col, core), at(1 - row, 1 - col, core)
        self.xs, self.ys, self.ds = at(row, 1 - col, 1 - core), at(1 - row, col, 1 - core), at(1 - row, 1 - col, 1 - core)


def remote(src, dst, send_sem, recv_sem, dev):
    return pltpu.make_async_remote_copy(src_ref=src, dst_ref=dst, send_sem=send_sem, recv_sem=recv_sem,
                                        device_id={"dp": dev}, device_id_type=pl.DeviceIdType.MESH)


def greet(devs):
    sem = pltpu.get_barrier_semaphore()
    for dev in devs:
        pl.semaphore_signal(sem, inc=1, device_id={"dp": dev}, device_id_type=pl.DeviceIdType.MESH)
    pl.semaphore_wait(sem, len(devs))


def gather_body(n, plan, n_in, n_out, *refs):
    ins, outs = refs[:n_in], refs[n_in:n_in + n_out]
    (stage, keep, gain_got, gain_row, raw, normed, load_sems, pack_sems, keep_sems, gain_send, gain_recv, row_sems, own_sems,
     send_sems, recv_sems) = refs[n_in + n_out:]
    at = Place()
    me = at.me
    gain_ref, hidden = ins[:2]
    gains_out, normed_out = outs[:2]
    jobs, pack_in, pack_out = plan(ins[2:], outs[2:], stage, keep)
    count = len(jobs)
    loads, taken = [], 0
    for pieces, _, _, _ in jobs:
        loads.append([pltpu.make_async_copy(src, dst, load_sems.at[taken + i]) for i, (src, dst) in enumerate(pieces)])
        taken += len(pieces)
    for copy in sum(loads, []):
        copy.start()
    batch = hidden.shape[0]
    row_in = [pltpu.make_async_copy(hidden.at[i], raw.at[i % 2], row_sems.at[0, i]) for i in range(batch)]
    row_out = [pltpu.make_async_copy(normed.at[i % 2], normed_out.at[i], row_sems.at[1, i]) for i in range(batch)]
    pack_in = [pltpu.make_async_copy(src, dst, pack_sems.at[i]) for i, (src, dst) in enumerate(pack_in)]
    pack_out = [pltpu.make_async_copy(src, dst, keep_sems.at[i]) for i, (src, dst) in enumerate(pack_out)]
    peers = [lax.rem(me + j, n) for j in range(1, n)]
    greet(peers)

    def gain_to(j):
        return remote(gain_ref, gain_got.at[me], gain_send.at[j], gain_recv.at[me], peers[j])

    def gain_from(j):
        return remote(gain_ref, gain_got.at[peers[j]], gain_send.at[j], gain_recv.at[peers[j]], peers[j])

    def share_gains():
        for j in range(n - 1):
            gain_to(j).start()
        gain_got[me] = gain_ref[...]

    def normalize():
        for j in range(n - 1):
            gain_from(j).wait_recv()
            gain_from(j).wait_send()
        gains_out[...] = gain_got[...]
        width = gain_ref.shape[1]
        for i in range(n):
            gain_row[:, pl.ds(i * width, width)] = gain_got[i, pl.ds(0, 1)]
        block = 32
        for i in range(batch):
            row_in[i].wait()
            if i >= 2:
                row_out[i - 2].wait()

            def step(r, carry, i=i):
                rows = pl.ds(pl.multiple_of(r * block, block), block)
                normed[i % 2, rows] = rms_norm(raw[i % 2, rows], gain_row[...])
                return carry

            lax.fori_loop(0, raw.shape[1] // block, step, 0)
            row_out[i].start()
            if i + 2 < batch:
                row_in[i + 2].start()

    def hop(k, i):
        _, buf, full, half = jobs[i]
        route = (
            (buf, full(at.me), at.xn, full(at.xn)),
            (buf, full(at.me), at.yn, full(at.yn)),
            (buf, full(at.me), at.sib, full(at.sib)),
            (half(at.xn, 0), half(at.xn, 0), at.yn, half(at.dg, 0)),
            (half(at.yn, 1), half(at.yn, 1), at.xn, half(at.dg, 1)),
            (full(at.xn), full(at.xn), at.sib, full(at.xs)),
            (full(at.yn), full(at.yn), at.sib, full(at.ys)),
            (half(at.dg, 0), half(at.dg, 0), at.sib, half(at.ds, 0)),
            (half(at.dg, 1), half(at.dg, 1), at.sib, half(at.ds, 1)),
        )
        return route[k]

    def start(k, i):
        src, dst, dev, _ = hop(k, i)
        remote(src, dst, send_sems.at[k, i], recv_sems.at[k, i], dev).start()

    def arrived(k, i):
        src, _, dev, land = hop(k, i)
        remote(src, land, send_sems.at[k, i], recv_sems.at[k, i], dev).wait_recv()

    def sent(k, i):
        src, dst, dev, _ = hop(k, i)
        remote(src, dst, send_sems.at[k, i], recv_sems.at[k, i], dev).wait_send()

    def relay(i):
        arrived(0, i)
        start(3, i)
        start(5, i)
        arrived(1, i)
        start(4, i)
        start(6, i)

    def relay_diagonal(i):
        arrived(3, i)
        start(7, i)
        arrived(4, i)
        start(8, i)

    own = []
    for i, (_, buf, full, _) in enumerate(jobs):
        for copy in loads[i]:
            copy.wait()
        for k in range(3):
            start(k, i)
        own.append(pltpu.make_async_copy(buf, full(me), own_sems.at[i]))
        own[-1].start()
        if i == 0:
            share_gains()
            for copy in row_in[:2] + pack_in:
                copy.start()
        if i == 1:
            for copy in pack_in:
                copy.wait()
            for copy in pack_out:
                copy.start()
            normalize()
        if i >= 1:
            relay(i - 1)
        if i >= 2:
            relay_diagonal(i - 2)
    relay(count - 1)
    relay_diagonal(count - 2)
    relay_diagonal(count - 1)
    for i in range(count):
        for k in (2, 5, 6, 7, 8):
            arrived(k, i)
        for k in range(9):
            sent(k, i)
        own[i].wait()
    for copy in pack_out + row_out[-2:]:
        copy.wait()


def first_gather(gains, hidden, w_query, w_key, w_value, w_out, w_gate, w_up, w_down, n):
    hd, kd = w_query.shape[1:]
    d = w_out.shape[2]
    block = w_down.shape[1]
    rest = block - kd

    def plan(ins, outs, stage, keep):
        wq, wk, wv, wo, wg, wu, wd = ins
        gqkv, go, gg, gu, gd, pg, pd, pk, pv = outs
        cols, rows = stage
        kg, kdn, kk, kv = keep

        def by_columns(src, buf, first):
            column = lambda dev: pl.ds(pl.multiple_of(dev * kd, kd), kd)
            full = lambda dev: gqkv.at[pl.ds(first, hd), column(dev)]
            half = lambda dev, h: gqkv.at[pl.ds(first + h * (hd // 2), hd // 2), column(dev)]
            return [(src, buf)], buf, full, half

        def by_rows(pieces, buf, out):
            full = lambda dev: out.at[pl.ds(pl.multiple_of(dev * kd, kd), kd)]
            half = lambda dev, h: out.at[pl.ds(pl.multiple_of(dev * kd + h * (kd // 2), kd // 2), kd // 2)]
            return pieces, buf, full, half

        def blocks(w, first, size, buf):
            return [(w.at[0, :, pl.ds(e * block + first, size)], buf.at[:, pl.ds(e * size, size)]) for e in range(n)]

        jobs = [by_columns(w.at[0], cols.at[i], i * hd) for i, w in enumerate((wq, wk, wv))]
        jobs += [
            by_rows([(wo.at[0], rows.at[0])], rows.at[0], go),
            by_rows(blocks(wg, 0, kd, rows.at[1]), rows.at[1], gg), by_rows(blocks(wu, 0, kd, rows.at[2]), rows.at[2], gu),
            by_rows([(wd.at[0, pl.ds(0, kd)], rows.at[3])], rows.at[3], gd),
        ]
        pack_in = blocks(wg, kd, rest, kg.at[0]) + blocks(wu, kd, rest, kg.at[1])
        pack_in += [(wd.at[0, pl.ds(kd, rest)], kdn), (wk.at[1], kk), (wv.at[1], kv)]
        return jobs, pack_in, [(kg, pg), (kdn, pd), (kk, pk), (kv, pv)]

    count = 7
    shape = lambda *dims: jax.ShapeDtypeStruct(dims, BF16)
    outs = [jax.ShapeDtypeStruct((n,) + gains.shape, F32), shape(*hidden.shape)]
    outs += [shape(3 * hd, d)] + [shape(n * kd, d)] * 4
    outs += [shape(2, kd, n * rest), shape(rest, d), shape(hd, kd), shape(hd, kd)]
    batch, seq, _ = hidden.shape
    dma = pltpu.SemaphoreType.DMA
    return pl.pallas_call(
        functools.partial(gather_body, n, plan, 9, len(outs)),
        out_shape=outs,
        in_specs=[VM] + [HBM] * 8,
        out_specs=[VM] + [HBM] * (len(outs) - 1),
        scratch_shapes=[
            (pltpu.VMEM((3, hd, kd), BF16), pltpu.VMEM((4, kd, d), BF16)),
            (pltpu.VMEM((2, kd, n * rest), BF16), pltpu.VMEM((rest, d), BF16), pltpu.VMEM((hd, kd), BF16), pltpu.VMEM((hd, kd), BF16)),
            pltpu.VMEM((n,) + gains.shape, F32), pltpu.VMEM((1, d), F32),
            pltpu.VMEM((2, seq, d), BF16), pltpu.VMEM((2, seq, d), BF16),
            dma((5 + 2 * n,)), dma((2 * n + 3,)), dma((4,)), dma((n - 1,)), dma((n,)), dma((2, batch)),
            dma((count,)), dma((9, count)), dma((9, count)),
        ],
        compiler_params=params(48, 2),
        cost_estimate=cost(50_000_000_000, 50_000_000),
        name="first_gather",
    )(gains, hidden, w_query, w_key, w_value, w_out, w_gate, w_up, w_down)


GROUPS = 6
TABLE_STEP = 512


def tail_body(n, layer, o_ref, x_ref, gm_ref, gf_ref, wo_hbm, wg_hbm, wu_hbm, wd_hbm, emb_hbm, out_ref,
              wo, wg, wu, wd, emb, got, lhs, send, back, mid_ref, rows_ref, sib_send, sib_got, gate_send, gate_got, z_row, z_got, z_lhs,
              log_send, log_got, local_sems, pair_sems, send_sems, recv_sems):
    ex = Exchange(n, send_sems, recv_sems)
    me = ex.me
    pairs = ((wo_hbm.at[layer], wo), (wg_hbm.at[layer], wg), (wu_hbm.at[layer], wu), (wd_hbm.at[layer], wd), (emb_hbm, emb))
    loads = [pltpu.make_async_copy(src, dst, local_sems.at[i]) for i, (src, dst) in enumerate(pairs)]
    for load in loads:
        load.start()
    ex.barrier()

    x = spread(ex, 0, o_ref, got, lhs)
    loads[0].wait()
    mid = (x_ref[...] + reduce_rows(ex, 1, dot(x, wo[...]), send, back)).astype(BF16).astype(F32)
    mid_ref[...] = mid

    rows_ref[...] = rms_norm(mid, gm_ref[...]).astype(F32)
    x = spread(ex, 2, rows_ref, got, lhs)
    loads[1].wait()
    loads[2].wait()
    block = wd.shape[0]

    def gate_up(p):
        cols = pl.ds(pl.multiple_of(p * block, block), block)
        return dot(x, wg[:, cols]), dot(x, wu[:, cols])

    at = Place()
    across = (at.xs, at.ys, at.ds, at.sib)
    along = (at.xn, at.yn, at.dg, me)
    to_sib = [remote(sib_send.at[k], sib_got.at[k], pair_sems.at[0, k], pair_sems.at[1, k], at.sib) for k in range(4)]
    to_chip = [remote(gate_send.at[k], gate_got.at[k], pair_sems.at[2, k], pair_sems.at[3, k], along[k]) for k in range(3)]

    def pass_across(k):
        sib_send[k, 0], sib_send[k, 1] = gate_up(across[k])
        to_sib[k].start()

    def pass_along(k):
        gate, up = gate_up(along[k])
        to_sib[k].wait_recv()
        gate = gate + sib_got[k, 0]
        up = up + sib_got[k, 1]
        if along[k] is not me:
            gate_send[k, 0], gate_send[k, 1] = gate, up
            to_chip[k].start()
        return gate, up

    order = (2, 0, 1, 3)
    pass_across(order[0])
    for k, after in zip(order, order[1:]):
        pass_across(after)
        pass_along(k)
    gate, up = pass_along(order[-1])
    for k in range(3):
        to_chip[k].wait_recv()
        gate = gate + gate_got[k, 0]
        up = up + gate_got[k, 1]
    for copy in to_sib + to_chip:
        copy.wait_send()
    act = (gate * (1.0 / (1.0 + jnp.exp(-gate))) * up).astype(BF16)

    loads[3].wait()
    h = (mid_ref[...] + reduce_rows(ex, 4, dot(act, wd[...]), send, back)).astype(BF16).astype(F32)

    z_row[...] = rms_norm(h, gf_ref[...])
    rows = rows_ref.shape[0]
    ex.start(5, lambda j: z_row, z_got.at[me])
    z_got[me] = z_row[...]
    ex.wait(5, lambda j: z_row, lambda p: z_got.at[p])
    for i in range(n):
        z_lhs[pl.ds(i * rows, rows)] = z_got[i].astype(F32)
    z = z_lhs[...].astype(BF16)
    loads[4].wait()
    vocab = emb.shape[0]
    group = vocab // GROUPS
    for g in range(GROUPS):
        def step(c, carry):
            first = pl.multiple_of(g * group + c * TABLE_STEP, TABLE_STEP)
            part = dot_nt(z, emb[pl.ds(first, TABLE_STEP)])
            for i in range(n):
                log_send[i, :, pl.ds(first, TABLE_STEP)] = part[i * rows:(i + 1) * rows]
            return carry

        lax.fori_loop(0, group // TABLE_STEP, step, 0)
        src = lambda j, g=g: log_send.at[ex.peer(j), :, pl.ds(g * group, group)]
        dst = lambda p, g=g: log_got.at[:, pl.ds(pl.multiple_of(p * vocab + g * group, group), group)]
        ex.start(6 + g, src, dst(me))
    log_got[:, pl.ds(pl.multiple_of(me * vocab, vocab), vocab)] = log_send[me]
    for g in range(GROUPS):
        src = lambda j, g=g: log_send.at[ex.peer(j), :, pl.ds(g * group, group)]
        dst = lambda p, g=g: log_got.at[:, pl.ds(pl.multiple_of(p * vocab + g * group, group), group)]
        ex.wait(6 + g, src, dst)
    out_ref[...] = log_got[...]


def tail(o, x, gm, gf, w_out, w_gate, w_up, w_down, emb, layer, n):
    rows, d = x.shape
    kd, ffn, block, vocab = w_gate.shape[1], w_gate.shape[2], w_down.shape[1], emb.shape[0]
    stages = 6 + GROUPS
    weights = kd * d + 2 * kd * ffn + block * d + vocab * d
    return pl.pallas_call(
        functools.partial(tail_body, n, layer),
        out_shape=jax.ShapeDtypeStruct((rows, n * vocab), F32),
        in_specs=[VM, VM, VM, VM] + [HBM] * 5,
        out_specs=VM,
        scratch_shapes=[
            pltpu.VMEM((kd, d), BF16), pltpu.VMEM((kd, ffn), BF16), pltpu.VMEM((kd, ffn), BF16),
            pltpu.VMEM((block, d), BF16), pltpu.VMEM((vocab, d), BF16),
            pltpu.VMEM((n, rows, kd), F32), pltpu.VMEM((n * rows, kd), F32),
            pltpu.VMEM((n, rows, d), F32), pltpu.VMEM((n, rows, d), F32),
            pltpu.VMEM((rows, d), F32), pltpu.VMEM((rows, d), F32),
            pltpu.VMEM((4, 2, n * rows, block), F32), pltpu.VMEM((4, 2, n * rows, block), F32),
            pltpu.VMEM((3, 2, n * rows, block), F32), pltpu.VMEM((3, 2, n * rows, block), F32),
            pltpu.VMEM((rows, d), BF16), pltpu.VMEM((n, rows, d), BF16), pltpu.VMEM((n * rows, d), F32),
            pltpu.VMEM((n, rows, vocab), F32), pltpu.VMEM((rows, n * vocab), F32),
            pltpu.SemaphoreType.DMA((5,)), pltpu.SemaphoreType.DMA((4, 4)), pltpu.SemaphoreType.DMA((stages, n)), pltpu.SemaphoreType.DMA((stages, n)),
        ],
        compiler_params=params(58, 1),
        cost_estimate=cost(n * rows * weights, weights),
        name="tail",
    )(o, x, gm, gf, w_out, w_gate, w_up, w_down, emb)


def solution(mesh):
    row_spec = P(("part", "dp"))
    layer_spec = P(None, "dp")

    def device_step(hidden, prompt_lens, g_attn, w_query, w_key, w_value, w_out, g_mlp, w_gate, w_up, w_down, g_final, embedding):
        batch, seq_len, dim = hidden.shape
        heads, head_dim = w_query.shape[2], w_query.shape[3]
        n_dev = dim // w_query.shape[1]
        freqs = rope_frequencies(head_dim)
        angles = freqs[:, None] * np.arange(seq_len, dtype=np.float32)[None]
        cos_es, sin_es = jnp.asarray(np.cos(angles)), jnp.asarray(np.sin(angles))

        def headed(w):
            return w.transpose(0, 2, 3, 1).reshape(w.shape[0], heads * head_dim, -1)

        wq_t, wk_t, wv_t = headed(w_query), headed(w_key), headed(w_value)
        kd = dim // n_dev
        gains_loc = jnp.concatenate([g_attn, g_mlp, g_final[None], jnp.zeros((3, kd), BF16)], axis=0).astype(F32)
        gains, normed, gqkv, go, gg1, gup1, gd1, pg2, pd2, pk1, pv1 = first_gather(
            gains_loc, hidden, wq_t, wk_t, wv_t, w_out, w_gate, w_up, w_down, n_dev)
        gains = gains.transpose(1, 0, 2).reshape(8, dim)
        gu2 = lax.all_gather(pg2, "dp", axis=1, tiled=True)
        gd2 = lax.all_gather(pd2, "dp", axis=0, tiled=True)
        gk1 = lax.all_gather(pk1, "dp", axis=1, tiled=True)
        gv1 = lax.all_gather(pv1, "dp", axis=1, tiled=True)
        ga0, ga1, gm0, gm1, gf, *_ = gains
        hd = heads * head_dim

        lens = prompt_lens
        rope = (cos_es, sin_es, head_dim)
        rows = batch * seq_len
        q0, k_cache, v_cache = project(normed.reshape(rows, dim), gqkv, *rope, (True, True, False), (1, 2, 2), 0)
        attended = attention(lens, q0, k_cache, v_cache, head_dim)
        proj = jnp.einsum("bks,kd->bsd", attended, go, preferred_element_type=F32)
        mid = (hidden.astype(F32) + proj).astype(BF16)
        mid = mid.reshape(rows, dim)
        act, normed_mlp = gate_up(mid, gm0[None], (gg1, gup1), gg1.shape[1])
        part = down(act, gd1, rows)
        [act] = gate_up(normed_mlp, None, (gu2,), gu2.shape[2])
        h1 = down(act, gd2, BAND, (mid, part))

        last = lens - 1
        x = jnp.take_along_axis(h1.reshape(batch, seq_len, dim), last[:, None, None], axis=1, mode="clip")[:, 0]
        q1 = last_query(rms_norm(x, ga1).astype(F32), wq_t, 1, n_dev).reshape(batch, heads, head_dim)
        half = head_dim // 2
        turn = last.astype(F32)[:, None, None] * freqs
        cos_b, sin_b = jnp.cos(turn), jnp.sin(turn)
        low, high = q1[..., :half], q1[..., half:]
        q1 = jnp.concatenate([low * cos_b - high * sin_b, high * cos_b + low * sin_b], axis=-1).astype(BF16)
        own = np.arange(hd)[None, :] // head_dim == np.arange(heads)[:, None]
        q_diag = jnp.where(own[None], q1.reshape(batch, 1, hd), jnp.zeros((), BF16))

        k_cache, normed1 = project(h1, gk1, *rope, (True,), (2,), 1, k_cache, ga1[None])
        [v_cache] = project(normed1, gv1, *rope, (False,), (2,), 1, v_cache)

        o1 = last_attention(lens, q_diag, k_cache, v_cache, head_dim, 1)
        logits = tail(o1, x.astype(F32), gm1[None], gf[None], w_out, w_gate, w_up, w_down, embedding, 1, n_dev)

        def cache(c):
            return c.reshape(2, batch, heads, head_dim, seq_len).transpose(0, 1, 4, 2, 3)

        return cache(k_cache), cache(v_cache), logits

    cache_spec = P(None, ("part", "dp"))
    return jax.shard_map(
        device_step,
        mesh=mesh,
        in_specs=(row_spec, row_spec) + (layer_spec,) * 9 + (P("dp"), P("dp")),
        out_specs=(cache_spec, cache_spec, row_spec),
        check_vma=False,
    )
```
